256 devices in a mesh: seq: 64 (over x, z, core), head: 4 (over y).
Axes of the slice: x: 4, y: 4, z: 8, core: 2. Of those that a mesh axis runs over, the one named last changes fastest.
Arguments:
- queries: bfloat16 [8192, 128], P('seq'), may hold values from -6 to 6
- key_rows: bfloat16 [8192, 128], P('seq'), may hold values from -0.0078125 to 0.0078125
- values: bfloat16 [8192, 5120], P('seq', 'head'), may hold values from -6 to 6
- gate_rows: bfloat16 [8192, 5120], P('seq', 'head'), may hold values from -6 to 6
- log_decay: float32 [8192, 80], P('seq', 'head'), may hold values from -0.69 to 0
- skip_gain: float32 [80], P('head'), may hold values from 0.3 to 4.2
- lam_index: int32 [8192], P('seq'), may hold values from 0 to 63
- segments: int32 [8192], P('seq'), may hold values from 0 to 255, never falling along the last dimension, each value on 1 to 64 neighbouring positions
- lam_table: float32 [64, 8, 80], P(None, None, 'head'), may hold values from 0.2 to 2
- norm_gain: float32 [5120], P('head'), may hold values from 0.25 to 1.75
- out_proj: bfloat16 [5120, 2560], P('head', 'seq'), may hold values from -0.078125 to 0.078125
Outputs:
- mixer_out: bfloat16 [8192, 2560], P(('seq', 'head'))
The draws below stay inside these ranges and needn't reach their ends.
Inputs may be any that keep to these rules, and one draw needn't show every extreme that they name: `segments`: stretch numbers never fall along the sequence; each stretch has 1 to 64 tokens.
All inputs are finite; a program needn't handle non-finite values.
Results may differ from the reference program's by a relative error of at most 0.012.
Values may be sent and summed in bfloat16 or wider, within the bound.
No kernel may reach another device: no remote copies, remote signals or barrier semaphores. Data moves between devices by JAX's collectives and lax.ppermute only.
A program may use at most 128 MiB of HBM per device.

```python
import math
import jax
import jax.numpy as jnp
import numpy as np
from jax import lax

DM = 2560
HEAD_TOTAL = 80
HEAD_DIM = 64
STATE = 128
TOK_DEV = 128
CLASSES = 64
LOGS = 6
LEVELS = 8
DI = 5120
GROUP_COLS = 1280
TOKEN_TOTAL = 8192


def draw_log_decay(key, part):
    key_sequence = jax.random.split(jax.random.fold_in(key, 11), 7)
    fast_share = 0.35
    fast_heads = jax.random.bernoulli(key_sequence[0], fast_share, (HEAD_TOTAL,))
    fast_rate = jax.random.uniform(key_sequence[1], (HEAD_TOTAL,), jnp.float32, 1.0 / 50.0, 1.0 / 30.0)
    slow_total = jax.random.uniform(key_sequence[2], (HEAD_TOTAL,), jnp.float32, 0.05, 0.4)
    baseline_rate = jnp.where(fast_heads, fast_rate, slow_total / TOKEN_TOTAL)
    token_multiplier = jnp.exp(jax.random.uniform(key_sequence[3], (TOKEN_TOTAL, HEAD_TOTAL), jnp.float32, -math.log(2.0), math.log(2.0)))
    shard_multiplier = jnp.exp(jax.random.uniform(key_sequence[4], (TOKEN_TOTAL // TOK_DEV, HEAD_TOTAL), jnp.float32, -math.log(2.0), math.log(2.0)))
    shard_multiplier = jnp.repeat(shard_multiplier, TOK_DEV, axis=0)
    spike_positions = jax.random.randint(key_sequence[5], (2,), 0, TOKEN_TOTAL)
    spike_rows = jnp.any(jnp.arange(TOKEN_TOTAL, dtype=jnp.int32)[:, None] == spike_positions[None, :], axis=1)
    spike_loss = jnp.log(1.0 - jax.random.uniform(key_sequence[6], (TOKEN_TOTAL, HEAD_TOTAL), jnp.float32, 0.2, 0.45))
    final_result = -baseline_rate[None, :] * token_multiplier * shard_multiplier + jnp.where(spike_rows[:, None], spike_loss, 0.0)
    return jnp.maximum(final_result, -0.69).astype(jnp.float32)


def draw_skip_gain(key, part):
    base_gain = jnp.exp(jnp.linspace(math.log(0.5), math.log(2.5), HEAD_TOTAL))
    jitter = jax.random.uniform(jax.random.fold_in(key, 23), (HEAD_TOTAL,), jnp.float32, -0.3, 0.3)
    return (base_gain * jnp.exp(jitter)).astype(jnp.float32)


def with_ends(drawn, rng, least, top_value):
    index_at = [jax.random.randint(jax.random.fold_in(rng, axis), (), 0, length) for axis, length in enumerate(drawn.shape)]
    main_axis = drawn.shape.index(max(drawn.shape))
    beside = index_at[:main_axis] + [(index_at[main_axis] + 1) % drawn.shape[main_axis]] + index_at[main_axis + 1:]
    return drawn.at[tuple(index_at)].set(least).at[tuple(beside)].set(top_value)


def levels(rng, shape, pieces, least, top_value):
    level = 1.0
    for position, shards_of in pieces:
        steps = jax.random.uniform(jax.random.fold_in(jax.random.fold_in(rng, 6), position), (shards_of,), jnp.float32, least / len(pieces), top_value / len(pieces))
        level = level * jnp.repeat(jnp.exp(steps), shape[position] // shards_of).reshape((-1,) + (1,) * (len(shape) - 1 - position))
    return level


def length_profile(number_of, total, bound, lean):
    weights = [(1 << 20) // math.isqrt(standing ** lean) + 1 for standing in range(2, number_of + 1)]
    surplus, holding = total - bound - (number_of - 1), [1] * (number_of - 1)
    while surplus > 0:
        movable = [i for i in range(number_of - 1) if holding[i] < bound]
        whole, remaining = sum([weights[i] for i in movable]), surplus
        for i in movable:
            addition = min(bound - holding[i], max(1, remaining * weights[i] // whole), surplus)
            holding[i] = holding[i] + addition
            surplus = surplus - addition
    return np.array([bound] + holding)


def uneven(own_key, count, total, bound, lean):
    if count == 2:
        one = jax.random.randint(own_key, (), max(1, total - bound), min(bound, total - 1) + 1)
        return jnp.stack([one, total - one])
    sizes = jnp.asarray(length_profile(count, total, bound, lean), jnp.int32)
    twos = (count - 1) // 2
    giver, sink = sizes[1:1 + 2 * twos:2], sizes[2:2 + 2 * twos:2]
    room = jnp.minimum(giver - 1, bound - sink)
    passed = jax.random.randint(jax.random.fold_in(own_key, 1), (twos,), 0, 1 << 20) % (room + 1)
    sizes = sizes.at[1:1 + 2 * twos:2].set(giver - passed).at[2:2 + 2 * twos:2].set(sink + passed)
    return sizes[jax.random.permutation(jax.random.fold_in(own_key, 2), count)]


def centred(own_key, shape, deviation, reach, shards=(), kind=jnp.bfloat16):
    gain = levels(own_key, shape, shards, -0.22, 0.18) if shards else 1.0
    drawn = jax.random.normal(own_key, shape, jnp.float32) * deviation * gain
    return jnp.minimum(jnp.maximum(drawn, -reach), reach).astype(kind)


def setup_inputs(seed: int = 0) -> dict:
    key_list = jax.random.split(jax.random.key(seed), 12)
    return {
        "queries": centred(key_list[0], (TOKEN_TOTAL, STATE), 1.0, 6.0, ((0, 64),)),
        "key_rows": centred(key_list[1], (TOKEN_TOTAL, STATE), ((STATE * TOKEN_TOTAL // 2) ** -0.5), 0.0078125, ((0, 64),)),
        "values": centred(key_list[2], (TOKEN_TOTAL, DI), 1.0, 6.0, ((0, 64), (1, 4))),
        "gate_rows": centred(key_list[3], (TOKEN_TOTAL, DI), 1.0, 6.0, ((0, 64), (1, 4))),
        "log_decay": draw_log_decay(jax.random.fold_in(key_list[11], 71), 0),
        "skip_gain": draw_skip_gain(jax.random.fold_in(key_list[11], 71), 0),
        "lam_index": with_ends(jax.random.randint(key_list[6], (TOKEN_TOTAL,), 0, CLASSES), jax.random.fold_in(key_list[6], 1), 0, CLASSES - 1).astype(jnp.int32),
        "segments": jnp.searchsorted(jnp.cumsum(uneven(key_list[7], TOKEN_TOTAL // 32, TOKEN_TOTAL, 64, 1)), jnp.arange(TOKEN_TOTAL), side="right").astype(jnp.int32),
        "lam_table": jnp.clip(jnp.exp(math.log(2.0) - 2.3025851 * jax.random.uniform(key_list[8], (CLASSES, LEVELS, HEAD_TOTAL), jnp.float32) ** levels(key_list[8], (CLASSES, LEVELS, HEAD_TOTAL), ((2, 4),), -0.2, 0.2)), 0.2, 2.0),
        "norm_gain": jnp.clip(1.0 + 0.15 * jax.random.normal(key_list[9], (DI,), jnp.float32), 0.25, 1.75),
        "out_proj": centred(key_list[10], (DI, DM), DI ** -0.5, 0.078125, ((0, 4), (1, 64))),
    }


epsilon = 1e-05
highest = lax.Precision.HIGHEST

def level_up(group_bf, bounds, level_pos, head_dim):
    pair_count = group_bf.shape[0] // 2
    width = 2 ** level_pos
    upper_start = (2 * jnp.arange(pair_count, dtype=jnp.int32) + 1) * width
    span = bounds[upper_start + width] - bounds[upper_start]
    pairs = group_bf.reshape(pair_count, 2, group_bf.shape[1], group_bf.shape[2]).astype(jnp.float32)
    factor = jnp.repeat(jnp.exp(span), head_dim, axis=1)[:, None, :]
    return (pairs[:, 1] + factor * pairs[:, 0]).astype(jnp.bfloat16)

def reference(queries, key_rows, values, gate_rows, log_decay, skip_gain, lam_index, segments, lam_table, norm_gain, out_proj):
    shard_count = TOKEN_TOTAL // TOK_DEV
    q_all = queries.reshape(shard_count, TOK_DEV, STATE)
    k_all = key_rows.reshape(shard_count, TOK_DEV, STATE)
    v_all = values.reshape(shard_count, TOK_DEV, DI)
    z_all = gate_rows.reshape(shard_count, TOK_DEV, DI)
    cum_all = jnp.cumsum(log_decay.reshape(shard_count, TOK_DEV, HEAD_TOTAL), axis=1)
    onehot = (lam_index[:, None] == jnp.arange(CLASSES, dtype=jnp.int32)[None, :]).astype(jnp.float32)
    level_wts = jnp.dot(onehot, lam_table.reshape(CLASSES, LEVELS * HEAD_TOTAL), precision=highest)
    level_wts = level_wts.reshape(shard_count, TOK_DEV, LEVELS, HEAD_TOTAL)
    seg_all = segments.reshape(shard_count, TOK_DEV)

    def end_state(args):
        k_blk, v_blk, c_blk = args
        decay_end = jnp.repeat(jnp.exp(c_blk[-1][None, :] - c_blk), HEAD_DIM, axis=1)
        decayed = (v_blk.astype(jnp.float32) * decay_end).astype(jnp.bfloat16)
        return jnp.dot(k_blk.T, decayed, preferred_element_type=jnp.float32).astype(jnp.bfloat16)
    end_states = lax.map(end_state, (k_all, v_all, cum_all))
    bounds = jnp.concatenate([jnp.zeros((1, HEAD_TOTAL), jnp.float32), jnp.cumsum(cum_all[:, -1, :], axis=0)], axis=0)
    group_levels = [end_states]
    for level_pos in range(LOGS - 1):
        group_levels.append(level_up(group_levels[-1], bounds, level_pos, HEAD_DIM))
    shard_ids = jnp.arange(shard_count, dtype=jnp.int32)
    positions = jnp.arange(TOK_DEV, dtype=jnp.int32)
    causal = positions[:, None] >= positions[None, :]

    def shard_out(args):
        shard_pos, q_blk, k_blk, v_blk, z_blk, c_blk, w_blk, s_blk = args
        here_bound = bounds[shard_pos]
        bucket_list = []
        for level_pos in range(LOGS):
            is_upper = jnp.bitwise_and(jnp.right_shift(shard_pos, level_pos), 1) == 1
            group_idx = jnp.right_shift(shard_pos, level_pos)
            start_row = jnp.left_shift(group_idx, level_pos)
            sibling = lax.dynamic_index_in_dim(group_levels[level_pos], jnp.maximum(group_idx - 1, 0), 0, keepdims=False)
            factor = jnp.repeat(jnp.exp(here_bound - bounds[start_row]), HEAD_DIM)[None, :]
            bucket_list.append(jnp.where(is_upper, factor * sibling.astype(jnp.float32), 0.0))
        buckets = jnp.stack(bucket_list)
        scores = jnp.dot(q_blk, k_blk.T, preferred_element_type=jnp.float32)
        c_heads = c_blk.T
        log_gaps = jnp.where(causal[None], c_heads[:, :, None] - c_heads[:, None, :], -jnp.inf)
        same_seg = s_blk[:, None] == s_blk[None, :]
        level_w = jnp.where(same_seg[None], w_blk[:, 0, :].T[:, :, None], w_blk[:, 1, :].T[:, :, None])
        weights_bf = (scores[None] * jnp.exp(log_gaps) * level_w).astype(jnp.bfloat16)
        v_heads = v_blk.reshape(TOK_DEV, HEAD_TOTAL, HEAD_DIM)
        local_out = jnp.einsum('htj,jhp->thp', weights_bf.astype(jnp.float32), v_heads.astype(jnp.float32), precision=highest)
        local_out = local_out.reshape(TOK_DEV, DI)
        level_reads = jnp.einsum('tn,lnc->tlc', q_blk.astype(jnp.float32), buckets, precision=highest)
        read_wts = jnp.repeat(w_blk[:, 2:, :], HEAD_DIM, axis=2)
        cross_out = lax.optimization_barrier(jnp.sum(level_reads * read_wts, axis=1)) * jnp.repeat(jnp.exp(c_blk), HEAD_DIM, axis=1)
        mixer_sum = local_out + cross_out + jnp.repeat(skip_gain, HEAD_DIM)[None, :] * v_blk.astype(jnp.float32)
        gated = mixer_sum * jax.nn.silu(z_blk.astype(jnp.float32))
        inv_rms = lax.rsqrt(lax.optimization_barrier(jnp.mean(gated * gated, axis=1, keepdims=True)) + epsilon)
        return (gated * inv_rms * norm_gain[None, :]).astype(jnp.bfloat16)
    hidden = lax.map(shard_out, (shard_ids, q_all, k_all, v_all, z_all, cum_all, level_wts, seg_all))
    hidden = hidden.reshape(TOKEN_TOTAL, DI)
    total_out = jnp.zeros((TOKEN_TOTAL, DM), jnp.float32)
    for group_pos in range(DI // GROUP_COLS):
        low_col = group_pos * GROUP_COLS
        partial_value = jnp.dot(hidden[:, low_col:low_col + GROUP_COLS], out_proj[low_col:low_col + GROUP_COLS], preferred_element_type=jnp.float32)
        total_out = total_out + lax.optimization_barrier(partial_value.astype(jnp.bfloat16)).astype(jnp.float32)
    return total_out.astype(jnp.bfloat16)
```

```python
import jax
import jax.numpy as jnp
from jax import lax
from jax.sharding import Mesh
from jax.sharding import PartitionSpec as P

DI = 5120
EPS = 1e-05
NX, NZ = 4, 8
HEAD_DIM = 64
BF = jnp.bfloat16
F32 = jnp.float32


def split3(value):
    hi = lax.reduce_precision(value, 8, 7)
    rest = value - hi
    mid = lax.reduce_precision(rest, 8, 7)
    low = lax.reduce_precision(rest - mid, 8, 7)
    return hi.astype(BF), mid.astype(BF), low.astype(BF)


def rows_of_totals(totals):
    parts = jnp.stack(split3(totals))
    return jnp.pad(parts, ((0, 13), (0, 128 - parts.shape[1])))


def totals_of_rows(rows, heads):
    rows = rows.astype(F32)[:, :heads]
    return rows[0] + rows[1] + rows[2]


def flip(value, axis, mask, size):
    return lax.ppermute(value, axis, [(i, i ^ mask) for i in range(size)])


def expand(per_head):
    return jnp.repeat(per_head, HEAD_DIM)[:, None]


def merged(own, other, own_total, other_total, upper):
    own_factor = jnp.where(upper, 1.0, jnp.exp(other_total))
    other_factor = jnp.where(upper, jnp.exp(own_total), 1.0)
    return (expand(own_factor) * own.astype(F32) + expand(other_factor) * other.astype(F32)).astype(BF)


def in_order(own, other, index):
    first = index == 0
    return jnp.concatenate([jnp.where(first, own, other), jnp.where(first, other, own)], axis=0)


def gather_weights(out_proj):
    z = lax.axis_index("z")
    core = lax.axis_index("core")
    rows = out_proj.T
    other = flip(rows, "core", 1, 2)
    pair = in_order(rows, other, core)
    mine = lax.dynamic_slice_in_dim(pair, core * 640, 640, 1)
    slab = jnp.zeros((NZ * 80, 640), BF)
    slab = lax.dynamic_update_slice_in_dim(slab, mine, z * 80, 0)
    for step in range(1, NZ):
        piece = lax.ppermute(mine, "z", [(i, (i + step) % NZ) for i in range(NZ)])
        slab = lax.dynamic_update_slice_in_dim(slab, piece, ((z + NZ - step) % NZ) * 80, 0)
    own = [slab]
    for step in range(1, NX):
        own.append(lax.ppermute(slab, "x", [(i, (i + step) % NX) for i in range(NX)]))
    others = [flip(block, "core", 1, 2) for block in own]
    return own, others


def per_device(
    queries,
    key_rows,
    values,
    gate_rows,
    log_decay,
    skip_gain,
    lam_index,
    segments,
    lam_table,
    norm_gain,
    out_proj,
):
    tok, _ = queries.shape
    heads = log_decay.shape[1]
    cols = values.shape[1]
    classes, levels, _ = lam_table.shape
    x = lax.axis_index("x")
    z = lax.axis_index("z")
    core = lax.axis_index("core")
    own_w, other_w = gather_weights(out_proj)

    cum = jnp.cumsum(log_decay, axis=0)
    total = cum[-1]
    decayed = (
        values.astype(F32) * jnp.repeat(jnp.exp(total[None, :] - cum), HEAD_DIM, axis=1)
    ).astype(BF)
    state = lax.dot_general(decayed, key_rows, (((0,), (0,)), ((), ())), preferred_element_type=F32)
    state = state.astype(BF)

    got = flip(jnp.concatenate([state, rows_of_totals(total)], axis=0), "core", 1, 2)
    got_total = totals_of_rows(got[cols:], heads)
    bucket0 = got[:cols]
    upper0 = core == 1
    prefix = jnp.where(upper0, got_total, 0.0)
    prefixes = [jnp.zeros_like(total)]
    uppers = [upper0]
    half_heads = heads // 2
    half = cols // 2
    quarter = half // 2

    def half_of(per_head):
        return lax.dynamic_slice_in_dim(per_head, core * half_heads, half_heads, 0)

    s1 = merged(
        lax.dynamic_slice_in_dim(state, core * half, half, 0),
        lax.dynamic_slice_in_dim(got, core * half, half, 0),
        half_of(total),
        half_of(got_total),
        upper0,
    )
    total = total + got_total

    zq = z % 2
    upper = zq == 1

    def quarter_of(per_head):
        return lax.dynamic_slice_in_dim(per_head, core * half_heads + zq * (half_heads // 2), half_heads // 2, 0)

    keep = lax.dynamic_slice_in_dim(s1, zq * quarter, quarter, 0)
    give = lax.dynamic_slice_in_dim(s1, (1 - zq) * quarter, quarter, 0)
    got = flip(jnp.concatenate([give, rows_of_totals(total)], axis=0), "z", 1, NZ)
    got_total = totals_of_rows(got[quarter:], heads)
    side = lax.ppermute(s1[:quarter], "z", [(i, i + 1) for i in range(0, NZ, 2)])
    bucket1 = jnp.concatenate([side, got[:quarter]], axis=0)
    group = merged(keep, got[:quarter], quarter_of(total), quarter_of(got_total), upper)
    prefixes.append(prefix)
    uppers.append(upper)
    prefix = prefix + jnp.where(upper, got_total, 0.0)
    total = total + got_total

    quarters = []
    plan = (("z", 2, NZ, z), ("z", 4, NZ, z), ("x", 1, NX, x), ("x", 2, NX, x))
    for number, (axis, mask, size, index) in enumerate(plan):
        upper = (index & mask) != 0
        got = flip(jnp.concatenate([group, rows_of_totals(total)], axis=0), axis, mask, size)
        got_total = totals_of_rows(got[quarter:], heads)
        quarters.append(got[:quarter])
        if number + 1 < len(plan):
            group = merged(group, got[:quarter], quarter_of(total), quarter_of(got_total), upper)
        prefixes.append(prefix)
        uppers.append(upper)
        prefix = prefix + jnp.where(upper, got_total, 0.0)
        total = total + got_total

    early = jnp.concatenate(quarters[:3], axis=0)
    early_side = flip(early, "z", 1, NZ)
    early_halves = [bucket1]
    for number in range(3):
        rows = slice(number * quarter, (number + 1) * quarter)
        early_halves.append(in_order(early[rows], early_side[rows], zq))
    early_half = jnp.concatenate(early_halves, axis=0)
    early_other = flip(early_half, "core", 1, 2)
    buckets = [bucket0]
    for number in range(4):
        rows = slice(number * half, (number + 1) * half)
        buckets.append(in_order(early_half[rows], early_other[rows], core))
    late_half = in_order(quarters[3], flip(quarters[3], "z", 1, NZ), zq)
    buckets.append(in_order(late_half, flip(late_half, "core", 1, 2), core))

    onehot = (lam_index[:, None] == jnp.arange(classes, dtype=jnp.int32)[None, :]).astype(F32)
    level_wts = jnp.dot(
        onehot, lam_table.reshape(classes, levels * heads), precision=lax.Precision.HIGHEST
    ).reshape(tok, levels, heads)

    scores = lax.dot_general(queries, key_rows, (((1,), (1,)), ((), ())), preferred_element_type=F32)
    pos = jnp.arange(tok, dtype=jnp.int32)
    causal = pos[:, None] >= pos[None, :]
    cum_t = cum.T
    gaps = jnp.where(causal[None], cum_t[:, :, None] - cum_t[:, None, :], -jnp.inf)
    same = segments[:, None] == segments[None, :]
    level_w = jnp.where(
        same[None], level_wts[:, 0, :].T[:, :, None], level_wts[:, 1, :].T[:, :, None]
    )
    weights = (scores[None] * jnp.exp(gaps) * level_w).astype(BF)
    local_out = jnp.einsum(
        "htj,jhp->thp",
        weights,
        values.reshape(tok, heads, HEAD_DIM),
        preferred_element_type=F32,
    ).reshape(tok, cols)

    total_out = local_out + jnp.repeat(skip_gain, HEAD_DIM)[None, :] * values.astype(F32)
    for level, bucket in enumerate(buckets):
        read = lax.dot_general(queries, bucket, (((1,), (1,)), ((), ())), preferred_element_type=F32)
        weight = level_wts[:, 2 + level, :] * jnp.exp(cum + prefixes[level][None, :])
        weight = jnp.where(uppers[level], weight, 0.0)
        total_out = total_out + read * jnp.repeat(weight, HEAD_DIM, axis=1)
    gated = total_out * jax.nn.silu(gate_rows.astype(F32))
    square_sum = jnp.sum(gated * gated, axis=1)
    scaled = (gated * norm_gain[None, :]).astype(BF)
    mine = lax.dynamic_slice_in_dim(scaled, core * half, half, 1)
    rest = lax.dynamic_slice_in_dim(scaled, (1 - core) * half, half, 1)
    contract = (((1,), (1,)), ((), ()))
    blocks = [
        (
            lax.dot_general(mine, a, contract, preferred_element_type=F32)
            + lax.dot_general(rest, b, contract, preferred_element_type=F32)
        ).astype(BF)
        for a, b in zip(own_w, other_w)
    ]
    squares = jnp.pad(jnp.stack(split3(square_sum), axis=1), ((0, 0), (0, 125)))
    turned = [blocks[0], blocks[3], blocks[2], blocks[1]]
    sent = jnp.concatenate(turned + [squares], axis=1).reshape(4, tok // 4, -1)
    arrived = jnp.sum(lax.all_to_all(sent, "y", 0, 0, tiled=True).astype(F32), axis=0)
    width = own_w[0].shape[0] * NX
    squares = arrived[:, width] + arrived[:, width + 1] + arrived[:, width + 2]
    result = (arrived[:, :width] * lax.rsqrt(squares / DI + EPS)[:, None]).astype(BF)
    twice = jnp.concatenate([result, result], axis=1)
    return lax.dynamic_slice_in_dim(twice, ((NX - x) % NX) * (width // NX), width, 1)


def solution(mesh):
    inner = Mesh(mesh.devices.reshape(NX, NZ, 2, 4), ("x", "z", "core", "y"))
    seq = ("x", "z", "core")
    return jax.shard_map(
        per_device,
        mesh=inner,
        in_specs=(
            P(seq, None),
            P(seq, None),
            P(seq, "y"),
            P(seq, "y"),
            P(seq, "y"),
            P("y"),
            P(seq),
            P(seq),
            P(None, None, "y"),
            P("y"),
            P("y", seq),
        ),
        out_specs=P((*seq, "y"), None),
        check_vma=False,
    )
```

```python
import jax
import jax.numpy as jnp
from jax import lax
from jax.experimental import pallas as pl
from jax.experimental.pallas import tpu as pltpu
from jax.sharding import Mesh
from jax.sharding import PartitionSpec as P

DI = 5120
EPS = 1e-05
NX, NZ, NY = 4, 8, 4
TOK, COLS, HEADS, NST = 128, 1280, 20, 128
HALF, QUART = 640, 320
LANE = 128
BF = jnp.bfloat16
F32 = jnp.float32
I32 = jnp.int32
NT = (((1,), (1,)), ((), ()))
TN = (((0,), (0,)), ((), ()))


def flip(value, axis, mask, size):
    return lax.ppermute(value, axis, [(i, i ^ mask) for i in range(size)])


def shift(value, axis, step, size):
    return lax.ppermute(value, axis, [(i, (i + step) % size) for i in range(size)])


def call(body, place, args, outs, scratch=(), flops=10**8, vmem=4):
    return pl.pallas_call(
        body,
        out_shape=outs,
        in_specs=[pl.BlockSpec(memory_space=pltpu.SMEM)]
        + [pl.BlockSpec(memory_space=pltpu.VMEM)] * len(args),
        out_specs=[pl.BlockSpec(memory_space=pltpu.VMEM)] * len(outs),
        scratch_shapes=list(scratch),
        compiler_params=pltpu.CompilerParams(vmem_limit_bytes=vmem << 20),
        cost_estimate=pl.CostEstimate(flops=flops, bytes_accessed=1 << 20, transcendentals=0),
    )(place, *args)


def shaped(*shape, dtype=BF):
    return jax.ShapeDtypeStruct(shape, dtype)


def lanes():
    return lax.broadcasted_iota(I32, (TOK, LANE), 1)


def rows():
    return lax.broadcasted_iota(I32, (TOK, LANE), 0)


def two_heads(first, second, lane):
    return jnp.where(lane < 64, first, second)


def padded(value, width=LANE):
    zeros = jnp.zeros((value.shape[0], width - value.shape[1]), value.dtype)
    return jnp.concatenate([value, zeros], axis=1)


def put_totals(ref, at, size, totals):
    hi = totals.astype(BF)
    rest = totals - hi.astype(F32)
    mid = rest.astype(BF)
    low = (rest - mid.astype(F32)).astype(BF)
    ref[at : at + size, :] = hi
    ref[at + size : at + 2 * size, :] = mid
    ref[at + 2 * size : at + 3 * size, :] = low


def get_totals(ref, at, size):
    parts = ref[at : at + 3 * size, :].astype(F32)
    return parts[:size] + parts[size : 2 * size] + parts[2 * size :]


def state_kernel(place, values, keys, log_decay, msg, cum_ref):
    cum = padded(log_decay[...])
    row, lane = rows(), lanes()
    step = 1
    while step < TOK:
        cum = cum + jnp.where(row >= step, pltpu.roll(cum, step, 0), 0.0)
        step *= 2
    cum_ref[...] = cum
    total = cum[TOK - 1 : TOK, :]
    factor = jnp.exp(total - cum)
    spread = jnp.broadcast_to(total, (TOK, LANE))
    spread = jnp.where(lane < 10, spread, pltpu.roll(spread, 6, 1))
    spread = jnp.where((lane < 10) | ((lane >= 16) & (lane < 26)), spread, 0.0)
    put_totals(msg, COLS, 32, spread.T[:32])
    key = keys[...]
    for p in range(10):
        cols = slice(p * LANE, (p + 1) * LANE)
        wide = two_heads(factor[:, 2 * p : 2 * p + 1], factor[:, 2 * p + 1 : 2 * p + 2], lane)
        decayed = (values[:, cols].astype(F32) * wide).astype(BF)
        msg[cols, :] = lax.dot_general(decayed, key, TN, preferred_element_type=F32).astype(BF)


def pair_kernel(place, own, got, msg, prefix):
    core = place[0]
    own_total = get_totals(own, COLS, 32)
    got_total = get_totals(got, COLS, 32)
    own_total = jnp.where(core == 0, own_total[:16], own_total[16:])
    got_total = jnp.where(core == 0, got_total[:16], got_total[16:])
    upper = core == 1
    own_factor = jnp.where(upper, 1.0, jnp.exp(got_total))
    got_factor = jnp.where(upper, jnp.exp(own_total), 1.0)
    put_totals(msg, HALF, 16, own_total + got_total)
    prefix[...] = jnp.where(upper, got_total, own_total)
    for h in range(10):
        at = pl.ds(pl.multiple_of(core * HALF + h * 64, 64), 64)
        merged = own_factor[h : h + 1] * own[at, :].astype(F32) + got_factor[h : h + 1] * got[at, :].astype(F32)
        msg[h * 64 : h * 64 + 64, :] = merged.astype(BF)


def chip_kernel(place, own, got, msg, prefix):
    zq = lax.rem(place[3], 2)
    upper = zq == 1
    own_total = get_totals(own, HALF, 16)
    got_total = get_totals(got, HALF, 16)
    own_factor = jnp.where(upper, 1.0, jnp.exp(got_total))
    got_factor = jnp.where(upper, jnp.exp(own_total), 1.0)
    put_totals(msg, QUART, 16, own_total + got_total)
    prefix[...] = jnp.where(upper, got_total, 0.0)
    for k in range(5):
        at = pl.ds(pl.multiple_of(zq * QUART + k * 64, 64), 64)
        own_f = jnp.where(zq == 0, own_factor[k : k + 1], own_factor[k + 5 : k + 6])
        got_f = jnp.where(zq == 0, got_factor[k : k + 1], got_factor[k + 5 : k + 6])
        merged = own_f * own[at, :].astype(F32) + got_f * got[at, :].astype(F32)
        msg[k * 64 : k * 64 + 64, :] = merged.astype(BF)


def merge_kernel(bit, place, own, got, old, msg, prefix):
    zq = lax.rem(place[3], 2)
    upper = lax.rem(place[3] // bit, 2) == 1
    own_total = get_totals(own, QUART, 16)
    got_total = get_totals(got, QUART, 16)
    own_factor = jnp.where(upper, 1.0, jnp.exp(got_total))
    got_factor = jnp.where(upper, jnp.exp(own_total), 1.0)
    put_totals(msg, QUART, 16, own_total + got_total)
    prefix[...] = old[...] + jnp.where(upper, got_total, 0.0)
    for k in range(5):
        at = slice(k * 64, k * 64 + 64)
        own_f = jnp.where(zq == 0, own_factor[k : k + 1], own_factor[k + 5 : k + 6])
        got_f = jnp.where(zq == 0, got_factor[k : k + 1], got_factor[k + 5 : k + 6])
        msg[at, :] = (own_f * own[at, :].astype(F32) + got_f * got[at, :].astype(F32)).astype(BF)


def merge_side_kernel(bit, place, own, got, old, before, msg, prefix, side):
    merge_kernel(bit, place, own, got, old, msg, prefix)
    side[:QUART, :] = before[:QUART, :]
    side[QUART:, :] = got[:QUART, :]


def lines_kernel(place, r1, r2, r3, old, late, prefix):
    zq = lax.rem(place[3], 2)
    odd = lax.rem(place[2], 2) == 1
    t1 = get_totals(r1, QUART, 16)
    t2 = get_totals(r2, QUART, 16)
    t3 = get_totals(r3, QUART, 16)
    prefix[...] = old[...] + jnp.where(odd, t1, 0.0)
    late[:QUART, :] = r1[:QUART, :]
    f2 = jnp.where(odd, 1.0, jnp.exp(t3))
    f3 = jnp.where(odd, jnp.exp(t2), 1.0)
    for k in range(5):
        at = slice(k * 64, k * 64 + 64)
        a = jnp.where(zq == 0, f2[k : k + 1], f2[k + 5 : k + 6])
        b = jnp.where(zq == 0, f3[k : k + 1], f3[k + 5 : k + 6])
        late[QUART + k * 64 : QUART + k * 64 + 64, :] = (
            a * r2[at, :].astype(F32) + b * r3[at, :].astype(F32)
        ).astype(BF)


def local_kernel(
    place, queries, keys, values, cum_ref, lam_index, segments, lam_table, skip, got, base, factors, mail
):
    core = place[0]
    row, lane = rows(), lanes()
    cum = cum_ref[...]
    cum_t = cum.T
    grow = jnp.exp(cum)
    picks = lax.broadcasted_iota(I32, (64, TOK), 0)
    onehot = (picks == lam_index[...]).astype(F32).astype(BF)

    def level(number):
        table = padded(lam_table[:, number, :])
        hi = table.astype(BF)
        rest = table - hi.astype(F32)
        mid = rest.astype(BF)
        low = (rest - mid.astype(F32)).astype(BF)
        out = lax.dot_general(onehot, hi, TN, preferred_element_type=F32)
        out = out + lax.dot_general(onehot, mid, TN, preferred_element_type=F32)
        return out + lax.dot_general(onehot, low, TN, preferred_element_type=F32)

    mine = jnp.zeros((TOK, LANE), F32)
    theirs = jnp.zeros((TOK, LANE), F32)
    for number in range(5):
        value = level(3 + number) * grow
        there = (lane >= number * 16) & (lane < number * 16 + 10)
        to_first = pltpu.roll(value, number * 16, 1)
        to_second = pltpu.roll(value, (number * 16 + LANE - 10) % LANE, 1)
        mine = jnp.where(there, jnp.where(core == 0, to_first, to_second), mine)
        theirs = jnp.where(there, jnp.where(core == 0, to_second, to_first), theirs)
    factors[...] = mine
    mail[:TOK, :] = queries[...]
    hi = theirs.astype(BF)
    mail[TOK : 2 * TOK, :] = hi
    mail[2 * TOK :, :] = (theirs - hi.astype(F32)).astype(BF)

    zero_level = jnp.where(core == 1, level(2) * grow, 0.0)
    near, far = level(0), level(1)
    q = queries[...]
    scores = lax.dot_general(q, keys[...], NT, preferred_element_type=F32)
    seg_row = jnp.broadcast_to(segments[...].astype(F32), (TOK, LANE))
    same = seg_row == seg_row.T
    causal = row >= lane
    for p in range(10):
        cols = slice(p * LANE, (p + 1) * LANE)
        pieces = []
        for h in (2 * p, 2 * p + 1):
            gap = jnp.where(causal, cum[:, h : h + 1] - cum_t[h : h + 1, :], -1e30)
            weight = jnp.where(same, near[:, h : h + 1], far[:, h : h + 1])
            weight = (scores * jnp.exp(gap) * weight).astype(BF)
            pieces.append(
                jnp.dot(weight, values[:, h * 64 : h * 64 + 64], preferred_element_type=F32)
            )
        read = lax.dot_general(q, got[cols, :], NT, preferred_element_type=F32)
        read = read * two_heads(zero_level[:, 2 * p : 2 * p + 1], zero_level[:, 2 * p + 1 : 2 * p + 2], lane)
        gain = two_heads(skip[:, 2 * p : 2 * p + 1], skip[:, 2 * p + 1 : 2 * p + 2], lane)
        base[:, cols] = jnp.concatenate(pieces, axis=1) + read + gain * values[:, cols].astype(F32)


def level_weights(place, factors, mail, first_total, prefixes):
    core, x, z = place[0], place[2], place[3]
    lane = lanes()
    blocks = [jnp.zeros((16, LANE), F32)] + [p[...] for p in prefixes]
    blocks = blocks + [jnp.zeros((16, LANE), F32)] * (8 - len(blocks))
    chip = jnp.concatenate(blocks, axis=0).T
    first = jnp.concatenate([first_total[...]] * 8, axis=0).T
    uppers = [lax.rem(z, 2), lax.rem(z // 2, 2), lax.rem(z // 4, 2), lax.rem(x, 2), lax.rem(x // 2, 2)]
    on = jnp.zeros((TOK, LANE), F32)
    for number in range(5):
        there = (lane >= number * 16) & (lane < number * 16 + 10)
        on = jnp.where(there, uppers[number].astype(F32), on)
    own_chip = jnp.exp(chip + jnp.where(core == 1, first, 0.0)) * on
    other_chip = jnp.exp(chip + jnp.where(core == 1, 0.0, first)) * on
    other = mail[TOK : 2 * TOK, :].astype(F32) + mail[2 * TOK :, :].astype(F32)
    return factors[...] * own_chip, other * other_chip


def add_levels(numbers, place, tables, pairs, q_own, q_other, own_w, other_w, start, finish_own, finish_other):
    zq = lax.rem(place[3], 2)
    lane = lanes()
    tables = list(tables)
    for own_ref, other_ref in pairs:
        own_v, other_v = own_ref(), other_ref()
        tables.append(
            jnp.concatenate(
                [jnp.where(zq == 0, own_v, other_v), jnp.where(zq == 0, other_v, own_v)], axis=0
            )
        )
    for p in range(5):
        cols = slice(p * LANE, (p + 1) * LANE)
        acc_own, acc_other = start(cols)
        for number, table in zip(numbers, tables):
            a, b = number * 16 + 2 * p, number * 16 + 2 * p + 1
            piece = table[p * LANE : (p + 1) * LANE]
            read = lax.dot_general(q_own, piece, NT, preferred_element_type=F32)
            acc_own = acc_own + read * two_heads(own_w[:, a : a + 1], own_w[:, b : b + 1], lane)
            read = lax.dot_general(q_other, piece, NT, preferred_element_type=F32)
            acc_other = acc_other + read * two_heads(other_w[:, a : a + 1], other_w[:, b : b + 1], lane)
        finish_own(cols, acc_own)
        finish_other(cols, acc_other)


def rows_of(ref, start=0):
    return lambda: ref[start : start + QUART, :]


def cross_kernel(
    place, queries, factors, mail, first_total, p2, p3, p4, p5, got1, got2, got3, side, own, other, own_w, other_w
):
    mine, theirs = level_weights(place, factors, mail, first_total, [p2, p3, p4, p5])
    own_w[...] = mine
    other_w[...] = theirs
    zero = jnp.zeros((TOK, LANE), F32)

    def keep_own(cols, value):
        own[:, cols] = value

    def keep_other(cols, value):
        other[:, cols] = value

    pairs = [(rows_of(got2), rows_of(side)), (rows_of(got3), rows_of(side, QUART))]
    add_levels(
        (0, 1, 2), place, [got1[:HALF, :]], pairs, queries[...], mail[:TOK, :], mine, theirs,
        lambda cols: (zero, zero), keep_own, keep_other,
    )


def late_kernel(place, queries, mail, own_w, other_w, late, late_side, own_in, other_in, own, back):
    def keep_own(cols, value):
        own[:, cols] = value

    def keep_back(cols, value):
        back[:, cols] = value.astype(BF)

    pairs = [
        (rows_of(late), rows_of(late_side)),
        (rows_of(late, QUART), rows_of(late_side, QUART)),
    ]
    add_levels(
        (3, 4), place, [], pairs, queries[...], mail[:TOK, :], own_w[...], other_w[...],
        lambda cols: (own_in[:, cols], other_in[:, cols]), keep_own, keep_back,
    )


def project_kernel(place, base, own, back, gate, gain, *refs):
    core, y = place[0], place[1]
    w_refs, out_refs, y_ref = refs[:16], refs[16:20], refs[20]
    part = TOK // NY
    lane = lanes()
    squares = jnp.zeros((TOK, LANE), F32)
    for p in range(10):
        cols = slice(p * LANE, (p + 1) * LANE)
        inner = slice((p % 5) * LANE, (p % 5) * LANE + LANE)
        cross = jnp.where(core == p // 5, own[:, inner], back[:, inner].astype(F32))
        gated = base[:, cols] + cross
        v = gate[:, cols].astype(F32)
        gated = gated * (v / (1.0 + jnp.exp(-v)))
        squares = squares + gated * gated
        y_ref[:, cols] = (gated * gain[:, cols]).astype(BF)
    squares = jnp.sum(squares, axis=1, keepdims=True)
    hi = squares.astype(BF).astype(F32)
    mid = (squares - hi).astype(BF).astype(F32)
    low = squares - hi - mid
    squares = jnp.where(lane == 0, hi, jnp.where(lane == 1, mid, jnp.where(lane == 2, low, 0.0)))
    squares = squares.astype(BF)
    mine = pl.ds(pl.multiple_of(core * HALF, HALF), HALF)
    rest = pl.ds(pl.multiple_of((1 - core) * HALF, HALF), HALF)
    y_mine, y_rest = y_ref[:, mine], y_ref[:, rest]

    def store(d, cols, value):
        for owner in range(NY):

            @pl.when(lax.rem(y + d, NY) == owner)
            def _():
                out_refs[d][:, cols] = value[owner * part : (owner + 1) * part]

    for d in range(NY):
        store(d, slice(2560, 2688), squares)
    for block in range(4):
        mine_w = jnp.concatenate([w_refs[2 * block][...], w_refs[2 * block + 1][...]], axis=0)
        rest_w = jnp.concatenate([w_refs[8 + 2 * block][...], w_refs[9 + 2 * block][...]], axis=0)
        total = lax.dot_general(y_mine, mine_w, NT, preferred_element_type=F32)
        total = total + lax.dot_general(y_rest, rest_w, NT, preferred_element_type=F32)
        total = total.astype(BF)
        for d in range(NY):
            store(d, slice(block * HALF, (block + 1) * HALF), total)


def finish_kernel(place, a_ref, b_ref, c_ref, d_ref, out_ref):
    x, z = place[2], place[3]

    def total(cols):
        left = a_ref[:, cols].astype(F32) + b_ref[:, cols].astype(F32)
        return left + (c_ref[:, cols].astype(F32) + d_ref[:, cols].astype(F32))

    squares = total(slice(2560, 2688))
    squares = squares[:, 0:1] + squares[:, 1:2] + squares[:, 2:3]
    inv = lax.rsqrt(squares / DI + EPS)
    amount = lax.rem(z + (NZ - 2), NZ) * 80
    for block in range(4):
        part = total(slice(block * HALF, (block + 1) * HALF)) * inv
        part = pltpu.roll(part, amount, 1)
        at = pl.multiple_of(lax.rem(x + (NX - 1 + block), NX) * HALF, HALF)
        out_ref[:, pl.ds(at, HALF)] = part.astype(BF)


def gather_weights(out_proj):
    core = lax.axis_index("core")
    own_rows = out_proj.T
    other_rows = flip(own_rows, "core", 1, 2)
    first = core == 0
    pair = jnp.concatenate(
        [jnp.where(first, own_rows, other_rows), jnp.where(first, other_rows, own_rows)], axis=0
    )
    mine = lax.dynamic_slice_in_dim(pair, core * HALF, HALF, 1)
    below1 = shift(mine, "z", 1, NZ)
    above1 = shift(mine, "z", -1, NZ)
    below2 = shift(below1, "z", 1, NZ)
    above2 = shift(above1, "z", -1, NZ)
    below3 = shift(below2, "z", 1, NZ)
    above3 = shift(above2, "z", -1, NZ)
    above4 = shift(above3, "z", -1, NZ)
    near = joined(below2, below1, mine, above1)
    far = joined(above2, above3, above4, below3)
    near_left = shift(near, "x", 1, NX)
    near_right = shift(near, "x", -1, NX)
    far_left = shift(far, "x", 1, NX)
    far_right = shift(far, "x", -1, NX)
    near_across = shift(near_left, "x", 1, NX)
    far_across = shift(far_right, "x", -1, NX)
    own = [near_left, far_left, near, far, near_right, far_right, near_across, far_across]
    order = (2, 3, 0, 4, 6, 1, 5, 7)
    others = [None] * 8
    for at in order:
        others[at] = flip(own[at], "core", 1, 2)
    return own, others


def join_kernel(place, a, b, c, d, out):
    for number, ref in enumerate((a, b, c, d)):
        out[number * 80 : (number + 1) * 80, :] = ref[...]


def joined(*pieces):
    return call(join_kernel, jnp.zeros((1,), I32), pieces, [shaped(QUART, HALF)], flops=10**6)[0]


def mixer(
    queries, key_rows, values, gate_rows, log_decay, skip_gain, lam_index, segments, lam_table, norm_gain, out_proj
):
    places = [lax.axis_index(name) for name in ("core", "y", "x", "z")]
    place = jnp.stack(places).astype(I32)
    own_w, other_w = gather_weights(out_proj)
    state, cum = call(
        state_kernel, place, (values, key_rows, log_decay),
        [shaped(COLS + 96, NST), shaped(TOK, LANE, dtype=F32)],
        vmem=6,
    )
    got0 = flip(state, "core", 1, 2)
    quart = shaped(QUART + 48, NST)
    line = shaped(16, LANE, dtype=F32)
    msg1, first_total = call(pair_kernel, place, (state, got0), [shaped(HALF + 48, NST), line])
    got1 = flip(msg1, "z", 1, NZ)
    msg2, p2 = call(chip_kernel, place, (msg1, got1), [quart, line])
    got2 = flip(msg2, "z", 2, NZ)
    msg3, p3 = call(lambda *r: merge_kernel(2, *r), place, (msg2, got2, p2), [quart, line])
    got3 = flip(msg3, "z", 4, NZ)
    msg4, p4, side = call(
        lambda *r: merge_side_kernel(4, *r), place, (msg3, got3, p3, got2), [quart, line, shaped(HALF, NST)]
    )
    r1 = flip(msg4, "x", 1, NX)
    r3 = flip(msg4, "x", 3, NX)
    r2 = flip(msg4, "x", 2, NX)
    side = flip(side, "z", 1, NZ)

    base, factors, mail = call(
        local_kernel, place,
        (
            queries, key_rows, values, cum, lam_index.reshape(1, TOK), segments.reshape(1, TOK),
            lam_table, skip_gain.reshape(1, HEADS), got0,
        ),
        [shaped(TOK, COLS, dtype=F32), shaped(TOK, LANE, dtype=F32), shaped(3 * TOK, LANE)],
        flops=3 * 10**8,
        vmem=12,
    )
    mail = flip(mail, "core", 1, 2)
    half = shaped(TOK, HALF, dtype=F32)
    late, p5 = call(lines_kernel, place, (r1, r2, r3, p4), [shaped(HALF, NST), line])
    late_side = flip(late, "z", 1, NZ)
    square = shaped(TOK, LANE, dtype=F32)
    own_acc, other_acc, own_lw, other_lw = call(
        cross_kernel, place,
        (queries, factors, mail, first_total, p2, p3, p4, p5, got1, got2, got3, side),
        [half, half, square, square],
        vmem=8,
    )
    own_cross, back = call(
        late_kernel, place,
        (queries, mail, own_lw, other_lw, late, late_side, own_acc, other_acc),
        [half, shaped(TOK, HALF)],
        vmem=8,
    )
    back = flip(back, "core", 1, 2)
    parts = call(
        project_kernel, place,
        (base, own_cross, back, gate_rows, norm_gain.reshape(1, COLS), *own_w, *other_w),
        [shaped(TOK // NY, 2688)] * NY,
        scratch=[pltpu.VMEM((TOK, COLS), BF)],
        flops=10**9,
        vmem=24,
    )
    arrived = [parts[0]]
    for d in range(1, NY):
        arrived.append(shift(parts[d], "y", d, NY))
    return call(finish_kernel, place, arrived, [shaped(TOK // NY, 2560)])[0]


def solution(mesh):
    inner = Mesh(mesh.devices.reshape(NX, NZ, 2, NY), ("x", "z", "core", "y"))
    seq = ("x", "z", "core")
    return jax.shard_map(
        mixer,
        mesh=inner,
        in_specs=(
            P(seq, None),
            P(seq, None),
            P(seq, "y"),
            P(seq, "y"),
            P(seq, "y"),
            P("y"),
            P(seq),
            P(seq),
            P(None, None, "y"),
            P("y"),
            P("y", seq),
        ),
        out_specs=P((*seq, "y"), None),
        check_vma=False,
    )
```

```python
import jax
import jax.numpy as jnp
from jax import lax
from jax.experimental import pallas as pl
from jax.experimental.pallas import tpu as pltpu
from jax.sharding import Mesh
from jax.sharding import PartitionSpec as P

DI = 5120
EPS = 1e-05
NX, NZ, NY = 4, 8, 4
TOK, COLS, HEADS, NST = 128, 1280, 20, 128
HALF, QUART = 640, 320
LANE = 128
BF = jnp.bfloat16
F32 = jnp.float32
I32 = jnp.int32
NT = (((1,), (1,)), ((), ()))
TN = (((0,), (0,)), ((), ()))


def flip(value, axis, mask, size):
    return lax.ppermute(value, axis, [(i, i ^ mask) for i in range(size)])


def shift(value, axis, step, size):
    return lax.ppermute(value, axis, [(i, (i + step) % size) for i in range(size)])


def call(body, place, args, outs, scratch=(), flops=10**8, vmem=4):
    return pl.pallas_call(
        body,
        out_shape=outs,
        in_specs=[pl.BlockSpec(memory_space=pltpu.SMEM)]
        + [pl.BlockSpec(memory_space=pltpu.VMEM)] * len(args),
        out_specs=[pl.BlockSpec(memory_space=pltpu.VMEM)] * len(outs),
        scratch_shapes=list(scratch),
        compiler_params=pltpu.CompilerParams(vmem_limit_bytes=vmem << 20),
        cost_estimate=pl.CostEstimate(flops=flops, bytes_accessed=1 << 20, transcendentals=0),
    )(place, *args)


def shaped(*shape, dtype=BF):
    return jax.ShapeDtypeStruct(shape, dtype)


def lanes():
    return lax.broadcasted_iota(I32, (TOK, LANE), 1)


def rows():
    return lax.broadcasted_iota(I32, (TOK, LANE), 0)


def two_heads(first, second, lane):
    return jnp.where(lane < 64, first, second)


def put_totals(ref, at, size, totals):
    hi = totals.astype(BF)
    rest = totals - hi.astype(F32)
    mid = rest.astype(BF)
    low = (rest - mid.astype(F32)).astype(BF)
    ref[at : at + size, :] = hi
    ref[at + size : at + 2 * size, :] = mid
    ref[at + 2 * size : at + 3 * size, :] = low


def get_totals(ref, at, size):
    parts = ref[at : at + 3 * size, :].astype(F32)
    return parts[:size] + parts[size : 2 * size] + parts[2 * size :]


def state_kernel(place, values, keys, log_decay, msg, cum_ref):
    lane = lanes()
    cum = jnp.concatenate([log_decay[...], jnp.zeros((4, TOK), F32)], axis=0)
    step = 1
    while step < TOK:
        cum = cum + jnp.where(lane[:24] >= step, pltpu.roll(cum, step, 1), 0.0)
        step *= 2
    cum = jnp.concatenate([cum, jnp.zeros((TOK - 24, TOK), F32)], axis=0).T
    cum_ref[...] = cum
    total = cum[TOK - 1 : TOK, :]
    factor = jnp.exp(total - cum)
    spread = jnp.broadcast_to(total, (TOK, LANE))
    spread = jnp.where(lane < 10, spread, pltpu.roll(spread, 6, 1))
    spread = jnp.where((lane < 10) | ((lane >= 16) & (lane < 26)), spread, 0.0)
    put_totals(msg, COLS, 32, spread.T[:32])
    key = keys[...]
    for p in range(10):
        cols = slice(p * LANE, (p + 1) * LANE)
        wide = two_heads(factor[:, 2 * p : 2 * p + 1], factor[:, 2 * p + 1 : 2 * p + 2], lane)
        decayed = (values[:, cols].astype(F32) * wide).astype(BF)
        msg[cols, :] = lax.dot_general(decayed, key, TN, preferred_element_type=F32).astype(BF)


def pair_kernel(place, own, got, msg, prefix):
    core = place[0]
    own_total = get_totals(own, COLS, 32)
    got_total = get_totals(got, COLS, 32)
    own_total = jnp.where(core == 0, own_total[:16], own_total[16:])
    got_total = jnp.where(core == 0, got_total[:16], got_total[16:])
    upper = core == 1
    own_factor = jnp.where(upper, 1.0, jnp.exp(got_total))
    got_factor = jnp.where(upper, jnp.exp(own_total), 1.0)
    put_totals(msg, HALF, 16, own_total + got_total)
    prefix[...] = jnp.where(upper, got_total, own_total)
    for h in range(10):
        at = pl.ds(pl.multiple_of(core * HALF + h * 64, 64), 64)
        merged = own_factor[h : h + 1] * own[at, :].astype(F32) + got_factor[h : h + 1] * got[at, :].astype(F32)
        msg[h * 64 : h * 64 + 64, :] = merged.astype(BF)


def chip_kernel(place, own, got, msg, prefix):
    zq = lax.rem(place[3], 2)
    upper = zq == 1
    own_total = get_totals(own, HALF, 16)
    got_total = get_totals(got, HALF, 16)
    own_factor = jnp.where(upper, 1.0, jnp.exp(got_total))
    got_factor = jnp.where(upper, jnp.exp(own_total), 1.0)
    put_totals(msg, QUART, 16, own_total + got_total)
    prefix[...] = jnp.where(upper, got_total, 0.0)
    for k in range(5):
        at = pl.ds(pl.multiple_of(zq * QUART + k * 64, 64), 64)
        own_f = jnp.where(zq == 0, own_factor[k : k + 1], own_factor[k + 5 : k + 6])
        got_f = jnp.where(zq == 0, got_factor[k : k + 1], got_factor[k + 5 : k + 6])
        merged = own_f * own[at, :].astype(F32) + got_f * got[at, :].astype(F32)
        msg[k * 64 : k * 64 + 64, :] = merged.astype(BF)


def merge_kernel(bit, place, own, got, old, msg, prefix):
    zq = lax.rem(place[3], 2)
    upper = lax.rem(place[3] // bit, 2) == 1
    own_total = get_totals(own, QUART, 16)
    got_total = get_totals(got, QUART, 16)
    own_factor = jnp.where(upper, 1.0, jnp.exp(got_total))
    got_factor = jnp.where(upper, jnp.exp(own_total), 1.0)
    put_totals(msg, QUART, 16, own_total + got_total)
    prefix[...] = old[...] + jnp.where(upper, got_total, 0.0)
    for k in range(5):
        at = slice(k * 64, k * 64 + 64)
        own_f = jnp.where(zq == 0, own_factor[k : k + 1], own_factor[k + 5 : k + 6])
        got_f = jnp.where(zq == 0, got_factor[k : k + 1], got_factor[k + 5 : k + 6])
        msg[at, :] = (own_f * own[at, :].astype(F32) + got_f * got[at, :].astype(F32)).astype(BF)


def merge_side_kernel(bit, place, own, got, old, before, msg, prefix, side):
    merge_kernel(bit, place, own, got, old, msg, prefix)
    side[:QUART, :] = before[:QUART, :]
    side[QUART:, :] = got[:QUART, :]


def lines_kernel(place, r1, r2, r3, old, late, prefix):
    zq = lax.rem(place[3], 2)
    odd = lax.rem(place[2], 2) == 1
    t1 = get_totals(r1, QUART, 16)
    t2 = get_totals(r2, QUART, 16)
    t3 = get_totals(r3, QUART, 16)
    prefix[...] = old[...] + jnp.where(odd, t1, 0.0)
    late[:QUART, :] = r1[:QUART, :]
    f2 = jnp.where(odd, 1.0, jnp.exp(t3))
    f3 = jnp.where(odd, jnp.exp(t2), 1.0)
    for k in range(5):
        at = slice(k * 64, k * 64 + 64)
        a = jnp.where(zq == 0, f2[k : k + 1], f2[k + 5 : k + 6])
        b = jnp.where(zq == 0, f3[k : k + 1], f3[k + 5 : k + 6])
        late[QUART + k * 64 : QUART + k * 64 + 64, :] = (
            a * r2[at, :].astype(F32) + b * r3[at, :].astype(F32)
        ).astype(BF)


def local_kernel(
    place, queries, keys, values, cum_ref, lam_index, segments, lam_table, skip, got, base, factors, mail
):
    core = place[0]
    row, lane = rows(), lanes()
    cum = cum_ref[...]
    cum_t = cum.T
    grow = jnp.exp(cum)
    picks = lax.broadcasted_iota(I32, (64, TOK), 0)
    onehot = (picks == lam_index[...]).astype(F32).astype(BF)

    tables = []
    for first in (0, 4):
        table = [jnp.concatenate([lam_table[:, first + i, :], jnp.zeros((12, 64), F32)], axis=0) for i in range(4)]
        table = jnp.concatenate(table, axis=0)
        hi = table.astype(BF)
        rest = table - hi.astype(F32)
        mid = rest.astype(BF)
        low = (rest - mid.astype(F32)).astype(BF)
        out = jnp.dot(hi, onehot, preferred_element_type=F32)
        out = out + jnp.dot(mid, onehot, preferred_element_type=F32)
        out = out + jnp.dot(low, onehot, preferred_element_type=F32)
        tables.append(out.T)

    def level(number):
        return pltpu.roll(tables[number // 4], (LANE - 32 * (number % 4)) % LANE, 1)

    mine = jnp.zeros((TOK, LANE), F32)
    theirs = jnp.zeros((TOK, LANE), F32)
    for number in range(5):
        value = level(3 + number) * grow
        there = (lane >= number * 16) & (lane < number * 16 + 10)
        to_first = pltpu.roll(value, number * 16, 1)
        to_second = pltpu.roll(value, (number * 16 + LANE - 10) % LANE, 1)
        mine = jnp.where(there, jnp.where(core == 0, to_first, to_second), mine)
        theirs = jnp.where(there, jnp.where(core == 0, to_second, to_first), theirs)
    factors[...] = mine
    mail[:TOK, :] = queries[...]
    hi = theirs.astype(BF)
    mail[TOK : 2 * TOK, :] = hi
    mail[2 * TOK :, :] = (theirs - hi.astype(F32)).astype(BF)

    zero_level = jnp.where(core == 1, level(2) * grow, 0.0)
    near, far = level(0), level(1)
    q = queries[...]
    scores = lax.dot_general(q, keys[...], NT, preferred_element_type=F32)
    seg_row = jnp.broadcast_to(segments[...].astype(F32), (TOK, LANE))
    same = seg_row == seg_row.T
    causal = row >= lane
    for p in range(10):
        cols = slice(p * LANE, (p + 1) * LANE)
        pieces = []
        for h in (2 * p, 2 * p + 1):
            gap = jnp.where(causal, cum[:, h : h + 1] - cum_t[h : h + 1, :], -1e30)
            weight = jnp.where(same, near[:, h : h + 1], far[:, h : h + 1])
            weight = (scores * jnp.exp(gap) * weight).astype(BF)
            pieces.append(
                jnp.dot(weight, values[:, h * 64 : h * 64 + 64], preferred_element_type=F32)
            )
        read = lax.dot_general(q, got[cols, :], NT, preferred_element_type=F32)
        read = read * two_heads(zero_level[:, 2 * p : 2 * p + 1], zero_level[:, 2 * p + 1 : 2 * p + 2], lane)
        gain = two_heads(skip[:, 2 * p : 2 * p + 1], skip[:, 2 * p + 1 : 2 * p + 2], lane)
        base[:, cols] = jnp.concatenate(pieces, axis=1) + read + gain * values[:, cols].astype(F32)


def level_weights(place, factors, mail, first_total, prefixes):
    core, x, z = place[0], place[2], place[3]
    lane = lanes()
    blocks = [jnp.zeros((16, LANE), F32)] + [p[...] for p in prefixes]
    blocks = blocks + [jnp.zeros((16, LANE), F32)] * (8 - len(blocks))
    chip = jnp.concatenate(blocks, axis=0).T
    first = jnp.concatenate([first_total[...]] * 8, axis=0).T
    uppers = [lax.rem(z, 2), lax.rem(z // 2, 2), lax.rem(z // 4, 2), lax.rem(x, 2), lax.rem(x // 2, 2)]
    on = jnp.zeros((TOK, LANE), F32)
    for number in range(5):
        there = (lane >= number * 16) & (lane < number * 16 + 10)
        on = jnp.where(there, uppers[number].astype(F32), on)
    own_chip = jnp.exp(chip + jnp.where(core == 1, first, 0.0)) * on
    other_chip = jnp.exp(chip + jnp.where(core == 1, 0.0, first)) * on
    other = mail[TOK : 2 * TOK, :].astype(F32) + mail[2 * TOK :, :].astype(F32)
    return factors[...] * own_chip, other * other_chip


def add_levels(numbers, place, tables, pairs, q_own, q_other, own_w, other_w, start, finish_own, finish_other):
    zq = lax.rem(place[3], 2)
    lane = lanes()
    tables = list(tables)
    for own_ref, other_ref in pairs:
        own_v, other_v = own_ref(), other_ref()
        tables.append(
            jnp.concatenate(
                [jnp.where(zq == 0, own_v, other_v), jnp.where(zq == 0, other_v, own_v)], axis=0
            )
        )
    for p in range(5):
        cols = slice(p * LANE, (p + 1) * LANE)
        acc_own, acc_other = start(cols)
        for number, table in zip(numbers, tables):
            a, b = number * 16 + 2 * p, number * 16 + 2 * p + 1
            piece = table[p * LANE : (p + 1) * LANE]
            read = lax.dot_general(q_own, piece, NT, preferred_element_type=F32)
            acc_own = acc_own + read * two_heads(own_w[:, a : a + 1], own_w[:, b : b + 1], lane)
            read = lax.dot_general(q_other, piece, NT, preferred_element_type=F32)
            acc_other = acc_other + read * two_heads(other_w[:, a : a + 1], other_w[:, b : b + 1], lane)
        finish_own(cols, acc_own)
        finish_other(cols, acc_other)


def rows_of(ref, start=0):
    return lambda: ref[start : start + QUART, :]


def cross_kernel(
    place, queries, factors, mail, first_total, p2, p3, p4, p5, got1, got2, got3, side, own, other, own_w, other_w
):
    mine, theirs = level_weights(place, factors, mail, first_total, [p2, p3, p4, p5])
    own_w[...] = mine
    other_w[...] = theirs
    zero = jnp.zeros((TOK, LANE), F32)

    def keep_own(cols, value):
        own[:, cols] = value

    def keep_other(cols, value):
        other[:, cols] = value

    pairs = [(rows_of(got2), rows_of(side)), (rows_of(got3), rows_of(side, QUART))]
    add_levels(
        (0, 1, 2), place, [got1[:HALF, :]], pairs, queries[...], mail[:TOK, :], mine, theirs,
        lambda cols: (zero, zero), keep_own, keep_other,
    )


def late_kernel(place, queries, mail, own_w, other_w, late, late_side, own_in, other_in, own, back):
    def keep_own(cols, value):
        own[:, cols] = value

    def keep_back(cols, value):
        back[:, cols] = value.astype(BF)

    pairs = [
        (rows_of(late), rows_of(late_side)),
        (rows_of(late, QUART), rows_of(late_side, QUART)),
    ]
    add_levels(
        (3, 4), place, [], pairs, queries[...], mail[:TOK, :], own_w[...], other_w[...],
        lambda cols: (own_in[:, cols], other_in[:, cols]), keep_own, keep_back,
    )


def project_kernel(place, base, own, back, gate, gain, *refs):
    core, y = place[0], place[1]
    w_refs, out_refs, y_ref = refs[:16], refs[16:20], refs[20]
    part = TOK // NY
    lane = lanes()
    squares = jnp.zeros((TOK, LANE), F32)
    for p in range(10):
        cols = slice(p * LANE, (p + 1) * LANE)
        inner = slice((p % 5) * LANE, (p % 5) * LANE + LANE)
        cross = jnp.where(core == p // 5, own[:, inner], back[:, inner].astype(F32))
        gated = base[:, cols] + cross
        v = gate[:, cols].astype(F32)
        gated = gated * (v / (1.0 + jnp.exp(-v)))
        squares = squares + gated * gated
        y_ref[:, cols] = (gated * gain[p : p + 1, :]).astype(BF)
    squares = jnp.sum(squares, axis=1, keepdims=True)
    hi = squares.astype(BF).astype(F32)
    mid = (squares - hi).astype(BF).astype(F32)
    low = squares - hi - mid
    squares = jnp.where(lane == 0, hi, jnp.where(lane == 1, mid, jnp.where(lane == 2, low, 0.0)))
    squares = squares.astype(BF)
    mine = pl.ds(pl.multiple_of(core * HALF, HALF), HALF)
    rest = pl.ds(pl.multiple_of((1 - core) * HALF, HALF), HALF)
    y_mine, y_rest = y_ref[:, mine], y_ref[:, rest]

    def store(d, cols, value):
        for owner in range(NY):

            @pl.when((y ^ d) == owner)
            def _():
                out_refs[d][:, cols] = value[owner * part : (owner + 1) * part]

    for d in range(NY):
        store(d, slice(2560, 2688), squares)
    for block in range(4):
        mine_w = jnp.concatenate([w_refs[2 * block][...], w_refs[2 * block + 1][...]], axis=0)
        rest_w = jnp.concatenate([w_refs[8 + 2 * block][...], w_refs[9 + 2 * block][...]], axis=0)
        total = lax.dot_general(y_mine, mine_w, NT, preferred_element_type=F32)
        total = total + lax.dot_general(y_rest, rest_w, NT, preferred_element_type=F32)
        total = total.astype(BF)
        for d in range(NY):
            store(d, slice(block * HALF, (block + 1) * HALF), total)


def finish_kernel(place, a_ref, b_ref, c_ref, d_ref, out_ref):
    x, z = place[2], place[3]

    def total(cols):
        left = a_ref[:, cols].astype(F32) + b_ref[:, cols].astype(F32)
        return left + (c_ref[:, cols].astype(F32) + d_ref[:, cols].astype(F32))

    squares = total(slice(2560, 2688))
    squares = squares[:, 0:1] + squares[:, 1:2] + squares[:, 2:3]
    inv = lax.rsqrt(squares / DI + EPS)
    amount = lax.rem(z + (NZ - 2), NZ) * 80
    for block in range(4):
        part = total(slice(block * HALF, (block + 1) * HALF)) * inv
        part = pltpu.roll(part, amount, 1)
        at = pl.multiple_of((x ^ block) * HALF, HALF)
        out_ref[:, pl.ds(at, HALF)] = part.astype(BF)


def gather_weights(out_proj):
    core = lax.axis_index("core")
    own_rows = out_proj.T
    other_rows = flip(own_rows, "core", 1, 2)
    first = core == 0
    pair = jnp.concatenate(
        [jnp.where(first, own_rows, other_rows), jnp.where(first, other_rows, own_rows)], axis=0
    )
    mine = lax.dynamic_slice_in_dim(pair, core * HALF, HALF, 1)
    below1 = shift(mine, "z", 1, NZ)
    above1 = shift(mine, "z", -1, NZ)
    below2 = shift(below1, "z", 1, NZ)
    above2 = shift(above1, "z", -1, NZ)
    below3 = shift(below2, "z", 1, NZ)
    above3 = shift(above2, "z", -1, NZ)
    above4 = shift(above3, "z", -1, NZ)
    near = joined(below2, below1, mine, above1)
    far = joined(above2, above3, above4, below3)
    near_1 = flip(near, "x", 1, NX)
    near_3 = flip(near, "x", 3, NX)
    far_1 = flip(far, "x", 1, NX)
    far_3 = flip(far, "x", 3, NX)
    near_2 = flip(near_3, "x", 1, NX)
    far_2 = flip(far_1, "x", 3, NX)
    own = [near, far, near_1, far_1, near_2, far_2, near_3, far_3]
    order = (0, 1, 2, 6, 4, 3, 7, 5)
    others = [None] * 8
    for at in order:
        others[at] = flip(own[at], "core", 1, 2)
    return own, others


def join_kernel(place, a, b, c, d, out):
    for number, ref in enumerate((a, b, c, d)):
        out[number * 80 : (number + 1) * 80, :] = ref[...]


def joined(*pieces):
    return call(join_kernel, jnp.zeros((1,), I32), pieces, [shaped(QUART, HALF)], flops=10**6)[0]


def mixer(
    queries, key_rows, values, gate_rows, log_decay, skip_gain, lam_index, segments, lam_table, norm_gain, out_proj
):
    places = [lax.axis_index(name) for name in ("core", "y", "x", "z")]
    place = jnp.stack(places).astype(I32)
    own_w, other_w = gather_weights(out_proj)
    state, cum = call(
        state_kernel, place, (values, key_rows, log_decay.T),
        [shaped(COLS + 96, NST), shaped(TOK, LANE, dtype=F32)],
        vmem=6,
    )
    got0 = flip(state, "core", 1, 2)
    quart = shaped(QUART + 48, NST)
    line = shaped(16, LANE, dtype=F32)
    msg1, first_total = call(pair_kernel, place, (state, got0), [shaped(HALF + 48, NST), line])
    got1 = flip(msg1, "z", 1, NZ)
    msg2, p2 = call(chip_kernel, place, (msg1, got1), [quart, line])
    got2 = flip(msg2, "z", 2, NZ)
    msg3, p3 = call(lambda *r: merge_kernel(2, *r), place, (msg2, got2, p2), [quart, line])
    got3 = flip(msg3, "z", 6, NZ)
    msg4, p4, side = call(
        lambda *r: merge_side_kernel(4, *r), place, (msg3, got3, p3, got2), [quart, line, shaped(HALF, NST)]
    )
    r1 = flip(msg4, "x", 1, NX)
    r3 = flip(msg4, "x", 3, NX)
    r2 = flip(msg4, "x", 2, NX)
    side = flip(side, "z", 1, NZ)

    base, factors, mail = call(
        local_kernel, place,
        (
            queries, key_rows, values, cum, lam_index.reshape(1, TOK), segments.reshape(1, TOK),
            lam_table.transpose(2, 1, 0), skip_gain.reshape(1, HEADS), got0,
        ),
        [shaped(TOK, COLS, dtype=F32), shaped(TOK, LANE, dtype=F32), shaped(3 * TOK, LANE)],
        flops=3 * 10**8,
        vmem=12,
    )
    mail = flip(mail, "core", 1, 2)
    half = shaped(TOK, HALF, dtype=F32)
    late, p5 = call(lines_kernel, place, (r1, r2, r3, p4), [shaped(HALF, NST), line])
    late_side = flip(late, "z", 1, NZ)
    square = shaped(TOK, LANE, dtype=F32)
    own_acc, other_acc, own_lw, other_lw = call(
        cross_kernel, place,
        (queries, factors, mail, first_total, p2, p3, p4, p5, got1, got2, got3, side),
        [half, half, square, square],
        vmem=8,
    )
    own_cross, back = call(
        late_kernel, place,
        (queries, mail, own_lw, other_lw, late, late_side, own_acc, other_acc),
        [half, shaped(TOK, HALF)],
        vmem=8,
    )
    back = flip(back, "core", 1, 2)
    parts = call(
        project_kernel, place,
        (base, own_cross, back, gate_rows, norm_gain.reshape(10, LANE), *own_w, *other_w),
        [shaped(TOK // NY, 2688)] * NY,
        scratch=[pltpu.VMEM((TOK, COLS), BF)],
        flops=10**9,
        vmem=24,
    )
    arrived = [parts[0]]
    for d in (2, 1, 3):
        arrived.append(flip(parts[d], "y", d, NY))
    return call(finish_kernel, place, arrived, [shaped(TOK // NY, 2560)])[0]


def solution(mesh):
    inner = Mesh(mesh.devices.reshape(NX, NZ, 2, NY), ("x", "z", "core", "y"))
    seq = ("x", "z", "core")
    return jax.shard_map(
        mixer,
        mesh=inner,
        in_specs=(
            P(seq, None),
            P(seq, None),
            P(seq, "y"),
            P(seq, "y"),
            P(seq, "y"),
            P("y"),
            P(seq),
            P(seq),
            P(None, None, "y"),
            P("y"),
            P("y", seq),
        ),
        out_specs=P((*seq, "y"), None),
        check_vma=False,
    )
```

```python
import jax
import jax.numpy as jnp
from jax import lax
from jax.experimental import pallas as pl
from jax.experimental.pallas import tpu as pltpu
from jax.sharding import Mesh
from jax.sharding import PartitionSpec as P

DI = 5120
EPS = 1e-05
NX, NZ, NY = 4, 8, 4
TOK, COLS, HEADS, NST = 128, 1280, 20, 128
HALF, QUART = 640, 320
LANE = 128
BF = jnp.bfloat16
F32 = jnp.float32
I32 = jnp.int32
NT = (((1,), (1,)), ((), ()))
TN = (((0,), (0,)), ((), ()))


def flip(value, axis, mask, size):
    return lax.ppermute(value, axis, [(i, i ^ mask) for i in range(size)])


def shift(value, axis, step, size):
    return lax.ppermute(value, axis, [(i, (i + step) % size) for i in range(size)])


def call(body, place, args, outs, scratch=(), flops=10**8, vmem=4, space=pltpu.VMEM):
    return pl.pallas_call(
        body,
        out_shape=outs,
        in_specs=[pl.BlockSpec(memory_space=pltpu.SMEM)]
        + [pl.BlockSpec(memory_space=space)] * len(args),
        out_specs=[pl.BlockSpec(memory_space=pltpu.VMEM)] * len(outs),
        scratch_shapes=list(scratch),
        compiler_params=pltpu.CompilerParams(vmem_limit_bytes=vmem << 20),
        cost_estimate=pl.CostEstimate(flops=flops, bytes_accessed=1 << 20, transcendentals=0),
    )(place, *args)


def shaped(*shape, dtype=BF):
    return jax.ShapeDtypeStruct(shape, dtype)


def lanes():
    return lax.broadcasted_iota(I32, (TOK, LANE), 1)


def rows():
    return lax.broadcasted_iota(I32, (TOK, LANE), 0)


def two_heads(first, second, lane):
    return jnp.where(lane < 64, first, second)


def put_totals(ref, at, size, totals):
    hi = totals.astype(BF)
    rest = totals - hi.astype(F32)
    mid = rest.astype(BF)
    low = (rest - mid.astype(F32)).astype(BF)
    ref[at : at + size, :] = hi
    ref[at + size : at + 2 * size, :] = mid
    ref[at + 2 * size : at + 3 * size, :] = low


def get_totals(ref, at, size):
    parts = ref[at : at + 3 * size, :].astype(F32)
    return parts[:size] + parts[size : 2 * size] + parts[2 * size :]


def state_kernel(place, values_hbm, keys_hbm, decay_hbm, msg, cum_ref, values, keys, log_decay, sems):
    lane = lanes()
    copies = [
        pltpu.make_async_copy(decay_hbm, log_decay, sems.at[0]),
        pltpu.make_async_copy(keys_hbm, keys, sems.at[1]),
        pltpu.make_async_copy(values_hbm, values, sems.at[2]),
    ]
    for copy in copies:
        copy.start()
    copies[0].wait()
    cum = jnp.concatenate([log_decay[...], jnp.zeros((4, TOK), F32)], axis=0)
    step = 1
    while step < TOK:
        cum = cum + jnp.where(lane[:24] >= step, pltpu.roll(cum, step, 1), 0.0)
        step *= 2
    cum = jnp.concatenate([cum, jnp.zeros((TOK - 24, TOK), F32)], axis=0).T
    cum_ref[...] = cum
    total = cum[TOK - 1 : TOK, :]
    factor = jnp.exp(total - cum)
    spread = jnp.broadcast_to(total, (TOK, LANE))
    spread = jnp.where(lane < 10, spread, pltpu.roll(spread, 6, 1))
    spread = jnp.where((lane < 10) | ((lane >= 16) & (lane < 26)), spread, 0.0)
    put_totals(msg, COLS, 32, spread.T[:32])
    copies[1].wait()
    copies[2].wait()
    key = keys[...]
    for p in range(10):
        cols = slice(p * LANE, (p + 1) * LANE)
        wide = two_heads(factor[:, 2 * p : 2 * p + 1], factor[:, 2 * p + 1 : 2 * p + 2], lane)
        decayed = (values[:, cols].astype(F32) * wide).astype(BF)
        msg[cols, :] = lax.dot_general(decayed, key, TN, preferred_element_type=F32).astype(BF)


def pair_kernel(place, own, got, msg, prefix):
    core = place[0]
    own_total = get_totals(own, COLS, 32)
    got_total = get_totals(got, COLS, 32)
    own_total = jnp.where(core == 0, own_total[:16], own_total[16:])
    got_total = jnp.where(core == 0, got_total[:16], got_total[16:])
    upper = core == 1
    own_factor = jnp.where(upper, 1.0, jnp.exp(got_total))
    got_factor = jnp.where(upper, jnp.exp(own_total), 1.0)
    put_totals(msg, HALF, 16, own_total + got_total)
    prefix[...] = jnp.where(upper, got_total, own_total)
    for h in range(10):
        at = pl.ds(pl.multiple_of(core * HALF + h * 64, 64), 64)
        merged = own_factor[h : h + 1] * own[at, :].astype(F32) + got_factor[h : h + 1] * got[at, :].astype(F32)
        msg[h * 64 : h * 64 + 64, :] = merged.astype(BF)


def chip_kernel(place, own, got, msg, prefix):
    zq = lax.rem(place[3], 2)
    upper = zq == 1
    own_total = get_totals(own, HALF, 16)
    got_total = get_totals(got, HALF, 16)
    own_factor = jnp.where(upper, 1.0, jnp.exp(got_total))
    got_factor = jnp.where(upper, jnp.exp(own_total), 1.0)
    put_totals(msg, QUART, 16, own_total + got_total)
    prefix[...] = jnp.where(upper, got_total, 0.0)
    for k in range(5):
        at = pl.ds(pl.multiple_of(zq * QUART + k * 64, 64), 64)
        own_f = jnp.where(zq == 0, own_factor[k : k + 1], own_factor[k + 5 : k + 6])
        got_f = jnp.where(zq == 0, got_factor[k : k + 1], got_factor[k + 5 : k + 6])
        merged = own_f * own[at, :].astype(F32) + got_f * got[at, :].astype(F32)
        msg[k * 64 : k * 64 + 64, :] = merged.astype(BF)


def merge_kernel(bit, place, own, got, old, msg, prefix):
    zq = lax.rem(place[3], 2)
    upper = lax.rem(place[3] // bit, 2) == 1
    own_total = get_totals(own, QUART, 16)
    got_total = get_totals(got, QUART, 16)
    own_factor = jnp.where(upper, 1.0, jnp.exp(got_total))
    got_factor = jnp.where(upper, jnp.exp(own_total), 1.0)
    put_totals(msg, QUART, 16, own_total + got_total)
    prefix[...] = old[...] + jnp.where(upper, got_total, 0.0)
    for k in range(5):
        at = slice(k * 64, k * 64 + 64)
        own_f = jnp.where(zq == 0, own_factor[k : k + 1], own_factor[k + 5 : k + 6])
        got_f = jnp.where(zq == 0, got_factor[k : k + 1], got_factor[k + 5 : k + 6])
        msg[at, :] = (own_f * own[at, :].astype(F32) + got_f * got[at, :].astype(F32)).astype(BF)


def merge_side_kernel(bit, place, own, got, old, before, msg, prefix, side):
    merge_kernel(bit, place, own, got, old, msg, prefix)
    side[:QUART, :] = before[:QUART, :]
    side[QUART:, :] = got[:QUART, :]


def lines_kernel(place, r1, r2, r3, old, late, prefix):
    zq = lax.rem(place[3], 2)
    odd = lax.rem(place[2], 2) == 1
    t1 = get_totals(r1, QUART, 16)
    t2 = get_totals(r2, QUART, 16)
    t3 = get_totals(r3, QUART, 16)
    prefix[...] = old[...] + jnp.where(odd, t1, 0.0)
    late[:QUART, :] = r1[:QUART, :]
    f2 = jnp.where(odd, 1.0, jnp.exp(t3))
    f3 = jnp.where(odd, jnp.exp(t2), 1.0)
    for k in range(5):
        at = slice(k * 64, k * 64 + 64)
        a = jnp.where(zq == 0, f2[k : k + 1], f2[k + 5 : k + 6])
        b = jnp.where(zq == 0, f3[k : k + 1], f3[k + 5 : k + 6])
        late[QUART + k * 64 : QUART + k * 64 + 64, :] = (
            a * r2[at, :].astype(F32) + b * r3[at, :].astype(F32)
        ).astype(BF)


def local_kernel(
    place, queries, keys, values, cum_ref, lam_index, segments, lam_table, skip, got, base, factors, mail
):
    core = place[0]
    row, lane = rows(), lanes()
    cum = cum_ref[...]
    cum_t = cum.T
    grow = jnp.exp(cum)
    picks = lax.broadcasted_iota(I32, (64, TOK), 0)
    onehot = (picks == lam_index[...]).astype(F32).astype(BF)

    tables = []
    for first in (0, 4):
        table = [jnp.concatenate([lam_table[:, first + i, :], jnp.zeros((12, 64), F32)], axis=0) for i in range(4)]
        table = jnp.concatenate(table, axis=0)
        hi = table.astype(BF)
        rest = table - hi.astype(F32)
        mid = rest.astype(BF)
        low = (rest - mid.astype(F32)).astype(BF)
        out = jnp.dot(hi, onehot, preferred_element_type=F32)
        out = out + jnp.dot(mid, onehot, preferred_element_type=F32)
        out = out + jnp.dot(low, onehot, preferred_element_type=F32)
        tables.append(out.T)

    def level(number):
        return pltpu.roll(tables[number // 4], (LANE - 32 * (number % 4)) % LANE, 1)

    mine = jnp.zeros((TOK, LANE), F32)
    theirs = jnp.zeros((TOK, LANE), F32)
    for number in range(5):
        value = level(3 + number) * grow
        there = (lane >= number * 16) & (lane < number * 16 + 10)
        to_first = pltpu.roll(value, number * 16, 1)
        to_second = pltpu.roll(value, (number * 16 + LANE - 10) % LANE, 1)
        mine = jnp.where(there, jnp.where(core == 0, to_first, to_second), mine)
        theirs = jnp.where(there, jnp.where(core == 0, to_second, to_first), theirs)
    factors[...] = mine
    mail[:TOK, :] = queries[...]
    hi = theirs.astype(BF)
    mail[TOK : 2 * TOK, :] = hi
    mail[2 * TOK :, :] = (theirs - hi.astype(F32)).astype(BF)

    zero_level = jnp.where(core == 1, level(2) * grow, 0.0)
    near, far = level(0), level(1)
    q = queries[...]
    scores = lax.dot_general(q, keys[...], NT, preferred_element_type=F32)
    seg_row = jnp.broadcast_to(segments[...].astype(F32), (TOK, LANE))
    same = seg_row == seg_row.T
    causal = row >= lane
    for p in range(10):
        cols = slice(p * LANE, (p + 1) * LANE)
        pieces = []
        for h in (2 * p, 2 * p + 1):
            gap = jnp.where(causal, cum[:, h : h + 1] - cum_t[h : h + 1, :], -1e30)
            weight = jnp.where(same, near[:, h : h + 1], far[:, h : h + 1])
            weight = (scores * jnp.exp(gap) * weight).astype(BF)
            pieces.append(
                jnp.dot(weight, values[:, h * 64 : h * 64 + 64], preferred_element_type=F32)
            )
        read = lax.dot_general(q, got[cols, :], NT, preferred_element_type=F32)
        read = read * two_heads(zero_level[:, 2 * p : 2 * p + 1], zero_level[:, 2 * p + 1 : 2 * p + 2], lane)
        gain = two_heads(skip[:, 2 * p : 2 * p + 1], skip[:, 2 * p + 1 : 2 * p + 2], lane)
        base[:, cols] = jnp.concatenate(pieces, axis=1) + read + gain * values[:, cols].astype(F32)


def level_weights(place, factors, mail, first_total, prefixes):
    core, x, z = place[0], place[2], place[3]
    lane = lanes()
    blocks = [jnp.zeros((16, LANE), F32)] + [p[...] for p in prefixes]
    blocks = blocks + [jnp.zeros((16, LANE), F32)] * (8 - len(blocks))
    chip = jnp.concatenate(blocks, axis=0).T
    first = jnp.concatenate([first_total[...]] * 8, axis=0).T
    uppers = [lax.rem(z, 2), lax.rem(z // 2, 2), lax.rem(z // 4, 2), lax.rem(x, 2), lax.rem(x // 2, 2)]
    on = jnp.zeros((TOK, LANE), F32)
    for number in range(5):
        there = (lane >= number * 16) & (lane < number * 16 + 10)
        on = jnp.where(there, uppers[number].astype(F32), on)
    own_chip = jnp.exp(chip + jnp.where(core == 1, first, 0.0)) * on
    other_chip = jnp.exp(chip + jnp.where(core == 1, 0.0, first)) * on
    other = mail[TOK : 2 * TOK, :].astype(F32) + mail[2 * TOK :, :].astype(F32)
    return factors[...] * own_chip, other * other_chip


def add_levels(numbers, place, tables, pairs, q_own, q_other, own_w, other_w, start, finish_own, finish_other):
    zq = lax.rem(place[3], 2)
    lane = lanes()
    tables = list(tables)
    for own_ref, other_ref in pairs:
        own_v, other_v = own_ref(), other_ref()
        tables.append(
            jnp.concatenate(
                [jnp.where(zq == 0, own_v, other_v), jnp.where(zq == 0, other_v, own_v)], axis=0
            )
        )
    for p in range(5):
        cols = slice(p * LANE, (p + 1) * LANE)
        acc_own, acc_other = start(cols)
        for number, table in zip(numbers, tables):
            a, b = number * 16 + 2 * p, number * 16 + 2 * p + 1
            piece = table[p * LANE : (p + 1) * LANE]
            read = lax.dot_general(q_own, piece, NT, preferred_element_type=F32)
            acc_own = acc_own + read * two_heads(own_w[:, a : a + 1], own_w[:, b : b + 1], lane)
            read = lax.dot_general(q_other, piece, NT, preferred_element_type=F32)
            acc_other = acc_other + read * two_heads(other_w[:, a : a + 1], other_w[:, b : b + 1], lane)
        finish_own(cols, acc_own)
        finish_other(cols, acc_other)


def rows_of(ref, start=0):
    return lambda: ref[start : start + QUART, :]


def cross_kernel(
    place, queries, factors, mail, first_total, p2, p3, p4, p5, got1, got2, got3, side, own, other, own_w, other_w
):
    mine, theirs = level_weights(place, factors, mail, first_total, [p2, p3, p4, p5])
    own_w[...] = mine
    other_w[...] = theirs
    zero = jnp.zeros((TOK, LANE), F32)

    def keep_own(cols, value):
        own[:, cols] = value

    def keep_other(cols, value):
        other[:, cols] = value

    pairs = [(rows_of(got2), rows_of(side)), (rows_of(got3), rows_of(side, QUART))]
    add_levels(
        (0, 1, 2), place, [got1[:HALF, :]], pairs, queries[...], mail[:TOK, :], mine, theirs,
        lambda cols: (zero, zero), keep_own, keep_other,
    )


def late_kernel(place, queries, mail, own_w, other_w, late, late_side, own_in, other_in, own, back):
    def keep_own(cols, value):
        own[:, cols] = value

    def keep_back(cols, value):
        back[:, cols] = value.astype(BF)

    pairs = [
        (rows_of(late), rows_of(late_side)),
        (rows_of(late, QUART), rows_of(late_side, QUART)),
    ]
    add_levels(
        (3, 4), place, [], pairs, queries[...], mail[:TOK, :], own_w[...], other_w[...],
        lambda cols: (own_in[:, cols], other_in[:, cols]), keep_own, keep_back,
    )


def project_kernel(place, base, own, back, gate, gain, *refs):
    core, y = place[0], place[1]
    w_refs, out_refs, y_ref = refs[:16], refs[16:20], refs[20]
    part = TOK // NY
    lane = lanes()
    squares = jnp.zeros((TOK, LANE), F32)
    for p in range(10):
        cols = slice(p * LANE, (p + 1) * LANE)
        inner = slice((p % 5) * LANE, (p % 5) * LANE + LANE)
        cross = jnp.where(core == p // 5, own[:, inner], back[:, inner].astype(F32))
        gated = base[:, cols] + cross
        v = gate[:, cols].astype(F32)
        gated = gated * (v / (1.0 + jnp.exp(-v)))
        squares = squares + gated * gated
        y_ref[:, cols] = (gated * gain[p : p + 1, :]).astype(BF)
    squares = jnp.sum(squares, axis=1, keepdims=True)
    hi = squares.astype(BF).astype(F32)
    mid = (squares - hi).astype(BF).astype(F32)
    low = squares - hi - mid
    squares = jnp.where(lane == 0, hi, jnp.where(lane == 1, mid, jnp.where(lane == 2, low, 0.0)))
    squares = squares.astype(BF)
    mine = pl.ds(pl.multiple_of(core * HALF, HALF), HALF)
    rest = pl.ds(pl.multiple_of((1 - core) * HALF, HALF), HALF)
    y_mine, y_rest = y_ref[:, mine], y_ref[:, rest]

    def store(d, cols, value):
        for owner in range(NY):

            @pl.when((y ^ d) == owner)
            def _():
                out_refs[d][:, cols] = value[owner * part : (owner + 1) * part]

    for d in range(NY):
        store(d, slice(2560, 2688), squares)
    for block in range(4):
        mine_w = jnp.concatenate([w_refs[2 * block][...], w_refs[2 * block + 1][...]], axis=0)
        rest_w = jnp.concatenate([w_refs[8 + 2 * block][...], w_refs[9 + 2 * block][...]], axis=0)
        total = lax.dot_general(y_mine, mine_w, NT, preferred_element_type=F32)
        total = total + lax.dot_general(y_rest, rest_w, NT, preferred_element_type=F32)
        total = total.astype(BF)
        for d in range(NY):
            store(d, slice(block * HALF, (block + 1) * HALF), total)


def finish_kernel(place, a_ref, b_ref, c_ref, d_ref, out_ref):
    x, z = place[2], place[3]

    def total(cols):
        left = a_ref[:, cols].astype(F32) + b_ref[:, cols].astype(F32)
        return left + (c_ref[:, cols].astype(F32) + d_ref[:, cols].astype(F32))

    squares = total(slice(2560, 2688))
    squares = squares[:, 0:1] + squares[:, 1:2] + squares[:, 2:3]
    inv = lax.rsqrt(squares / DI + EPS)
    amount = lax.rem(z + (NZ - 2), NZ) * 80
    for block in range(4):
        part = total(slice(block * HALF, (block + 1) * HALF)) * inv
        part = pltpu.roll(part, amount, 1)
        at = pl.multiple_of((x ^ block) * HALF, HALF)
        out_ref[:, pl.ds(at, HALF)] = part.astype(BF)


def gather_weights(out_proj):
    core = lax.axis_index("core")
    own_rows = out_proj.T
    other_rows = flip(own_rows, "core", 1, 2)
    first = core == 0
    pair = jnp.concatenate(
        [jnp.where(first, own_rows, other_rows), jnp.where(first, other_rows, own_rows)], axis=0
    )
    mine = lax.dynamic_slice_in_dim(pair, core * HALF, HALF, 1)
    below1 = shift(mine, "z", 1, NZ)
    above1 = shift(mine, "z", -1, NZ)
    below2 = shift(below1, "z", 1, NZ)
    above2 = shift(above1, "z", -1, NZ)
    below3 = shift(below2, "z", 1, NZ)
    above3 = shift(above2, "z", -1, NZ)
    above4 = shift(above3, "z", -1, NZ)
    near = joined(below2, below1, mine, above1)
    far = joined(above2, above3, above4, below3)
    near_1 = flip(near, "x", 1, NX)
    near_3 = flip(near, "x", 3, NX)
    far_1 = flip(far, "x", 1, NX)
    far_3 = flip(far, "x", 3, NX)
    near_2 = flip(near_3, "x", 1, NX)
    far_2 = flip(far_1, "x", 3, NX)
    own = [near, far, near_1, far_1, near_2, far_2, near_3, far_3]
    order = (0, 1, 2, 6, 4, 3, 7, 5)
    others = [None] * 8
    for at in order:
        others[at] = flip(own[at], "core", 1, 2)
    return own, others


def join_kernel(place, a, b, c, d, out):
    for number, ref in enumerate((a, b, c, d)):
        out[number * 80 : (number + 1) * 80, :] = ref[...]


def joined(*pieces):
    return call(join_kernel, jnp.zeros((1,), I32), pieces, [shaped(QUART, HALF)], flops=10**6)[0]


def mixer(
    queries, key_rows, values, gate_rows, log_decay, skip_gain, lam_index, segments, lam_table, norm_gain, out_proj
):
    places = [lax.axis_index(name) for name in ("core", "y", "x", "z")]
    place = jnp.stack(places).astype(I32)
    own_w, other_w = gather_weights(out_proj)
    state, cum = call(
        state_kernel, place, (values, key_rows, log_decay.T),
        [shaped(COLS + 96, NST), shaped(TOK, LANE, dtype=F32)],
        scratch=[
            pltpu.VMEM((TOK, COLS), BF), pltpu.VMEM((TOK, NST), BF), pltpu.VMEM((HEADS, TOK), F32),
            pltpu.SemaphoreType.DMA((3,)),
        ],
        vmem=6,
        space=pltpu.HBM,
    )
    got0 = flip(state, "core", 1, 2)
    quart = shaped(QUART + 48, NST)
    line = shaped(16, LANE, dtype=F32)
    msg1, first_total = call(pair_kernel, place, (state, got0), [shaped(HALF + 48, NST), line])
    got1 = flip(msg1, "z", 1, NZ)
    msg2, p2 = call(chip_kernel, place, (msg1, got1), [quart, line])
    got2 = flip(msg2, "z", 2, NZ)
    msg3, p3 = call(lambda *r: merge_kernel(2, *r), place, (msg2, got2, p2), [quart, line])
    got3 = flip(msg3, "z", 6, NZ)
    msg4, p4, side = call(
        lambda *r: merge_side_kernel(4, *r), place, (msg3, got3, p3, got2), [quart, line, shaped(HALF, NST)]
    )
    r1 = flip(msg4, "x", 1, NX)
    r3 = flip(msg4, "x", 3, NX)
    r2 = flip(msg4, "x", 2, NX)
    side = flip(side, "z", 1, NZ)

    base, factors, mail = call(
        local_kernel, place,
        (
            queries, key_rows, values, cum, lam_index.reshape(1, TOK), segments.reshape(1, TOK),
            lam_table.transpose(2, 1, 0), skip_gain.reshape(1, HEADS), got0,
        ),
        [shaped(TOK, COLS, dtype=F32), shaped(TOK, LANE, dtype=F32), shaped(3 * TOK, LANE)],
        flops=3 * 10**8,
        vmem=12,
    )
    mail = flip(mail, "core", 1, 2)
    half = shaped(TOK, HALF, dtype=F32)
    late, p5 = call(lines_kernel, place, (r1, r2, r3, p4), [shaped(HALF, NST), line])
    late_side = flip(late, "z", 1, NZ)
    square = shaped(TOK, LANE, dtype=F32)
    own_acc, other_acc, own_lw, other_lw = call(
        cross_kernel, place,
        (queries, factors, mail, first_total, p2, p3, p4, p5, got1, got2, got3, side),
        [half, half, square, square],
        vmem=8,
    )
    own_cross, back = call(
        late_kernel, place,
        (queries, mail, own_lw, other_lw, late, late_side, own_acc, other_acc),
        [half, shaped(TOK, HALF)],
        vmem=8,
    )
    back = flip(back, "core", 1, 2)
    parts = call(
        project_kernel, place,
        (base, own_cross, back, gate_rows, norm_gain.reshape(10, LANE), *own_w, *other_w),
        [shaped(TOK // NY, 2688)] * NY,
        scratch=[pltpu.VMEM((TOK, COLS), BF)],
        flops=10**9,
        vmem=24,
    )
    arrived = [parts[0]]
    for d in (2, 1, 3):
        arrived.append(flip(parts[d], "y", d, NY))
    return call(finish_kernel, place, arrived, [shaped(TOK // NY, 2560)])[0]


def solution(mesh):
    inner = Mesh(mesh.devices.reshape(NX, NZ, 2, NY), ("x", "z", "core", "y"))
    seq = ("x", "z", "core")
    return jax.shard_map(
        mixer,
        mesh=inner,
        in_specs=(
            P(seq, None),
            P(seq, None),
            P(seq, "y"),
            P(seq, "y"),
            P(seq, "y"),
            P("y"),
            P(seq),
            P(seq),
            P(None, None, "y"),
            P("y"),
            P("y", seq),
        ),
        out_specs=P((*seq, "y"), None),
        check_vma=False,
    )
```

```python
import jax
import jax.numpy as jnp
from jax import lax
from jax.experimental import pallas as pl
from jax.experimental.pallas import tpu as pltpu
from jax.sharding import Mesh
from jax.sharding import PartitionSpec as P

DI = 5120
EPS = 1e-05
NX, NZ, NY = 4, 8, 4
TOK, COLS, HEADS, NST = 128, 1280, 20, 128
HALF, QUART = 640, 320
LANE = 128
BF = jnp.bfloat16
F32 = jnp.float32
I32 = jnp.int32
NT = (((1,), (1,)), ((), ()))
TN = (((0,), (0,)), ((), ()))


def flip(value, axis, mask, size):
    return lax.ppermute(value, axis, [(i, i ^ mask) for i in range(size)])


def shift(value, axis, step, size):
    return lax.ppermute(value, axis, [(i, (i + step) % size) for i in range(size)])


def call(body, place, args, outs, scratch=(), flops=10**8, vmem=4):
    return pl.pallas_call(
        body,
        out_shape=outs,
        in_specs=[pl.BlockSpec(memory_space=pltpu.SMEM)]
        + [pl.BlockSpec(memory_space=pltpu.VMEM)] * len(args),
        out_specs=[pl.BlockSpec(memory_space=pltpu.VMEM)] * len(outs),
        scratch_shapes=list(scratch),
        compiler_params=pltpu.CompilerParams(vmem_limit_bytes=vmem << 20),
        cost_estimate=pl.CostEstimate(flops=flops, bytes_accessed=1 << 20, transcendentals=0),
    )(place, *args)


def shaped(*shape, dtype=BF):
    return jax.ShapeDtypeStruct(shape, dtype)


def lanes():
    return lax.broadcasted_iota(I32, (TOK, LANE), 1)


def rows():
    return lax.broadcasted_iota(I32, (TOK, LANE), 0)


def two_heads(first, second, lane):
    return jnp.where(lane < 64, first, second)


def put_totals(ref, at, size, totals):
    hi = totals.astype(BF)
    rest = totals - hi.astype(F32)
    mid = rest.astype(BF)
    low = (rest - mid.astype(F32)).astype(BF)
    ref[at : at + size, :] = hi
    ref[at + size : at + 2 * size, :] = mid
    ref[at + 2 * size : at + 3 * size, :] = low


def get_totals(ref, at, size):
    parts = ref[at : at + 3 * size, :].astype(F32)
    return parts[:size] + parts[size : 2 * size] + parts[2 * size :]


def state_kernel(place, values, keys, log_decay, msg, cum_ref):
    lane = lanes()
    cum = jnp.concatenate([log_decay[...], jnp.zeros((4, TOK), F32)], axis=0)
    step = 1
    while step < TOK:
        cum = cum + jnp.where(lane[:24] >= step, pltpu.roll(cum, step, 1), 0.0)
        step *= 2
    cum = jnp.concatenate([cum, jnp.zeros((TOK - 24, TOK), F32)], axis=0).T
    cum_ref[...] = cum
    total = cum[TOK - 1 : TOK, :]
    factor = jnp.exp(total - cum)
    spread = jnp.broadcast_to(total, (TOK, LANE))
    spread = jnp.where(lane < 10, spread, pltpu.roll(spread, 6, 1))
    spread = jnp.where((lane < 10) | ((lane >= 16) & (lane < 26)), spread, 0.0)
    put_totals(msg, COLS, 32, spread.T[:32])
    key = keys[...]
    for p in range(10):
        cols = slice(p * LANE, (p + 1) * LANE)
        wide = two_heads(factor[:, 2 * p : 2 * p + 1], factor[:, 2 * p + 1 : 2 * p + 2], lane)
        decayed = (values[:, cols].astype(F32) * wide).astype(BF)
        msg[cols, :] = lax.dot_general(decayed, key, TN, preferred_element_type=F32).astype(BF)


def pair_kernel(place, own, got, msg, prefix):
    core = place[0]
    own_total = get_totals(own, COLS, 32)
    got_total = get_totals(got, COLS, 32)
    own_total = jnp.where(core == 0, own_total[:16], own_total[16:])
    got_total = jnp.where(core == 0, got_total[:16], got_total[16:])
    upper = core == 1
    own_factor = jnp.where(upper, 1.0, jnp.exp(got_total))
    got_factor = jnp.where(upper, jnp.exp(own_total), 1.0)
    put_totals(msg, HALF, 16, own_total + got_total)
    prefix[...] = jnp.where(upper, got_total, own_total)
    for h in range(10):
        at = pl.ds(pl.multiple_of(core * HALF + h * 64, 64), 64)
        merged = own_factor[h : h + 1] * own[at, :].astype(F32) + got_factor[h : h + 1] * got[at, :].astype(F32)
        msg[h * 64 : h * 64 + 64, :] = merged.astype(BF)


def chip_kernel(place, own, got, msg, prefix):
    zq = lax.rem(place[3], 2)
    upper = zq == 1
    own_total = get_totals(own, HALF, 16)
    got_total = get_totals(got, HALF, 16)
    own_factor = jnp.where(upper, 1.0, jnp.exp(got_total))
    got_factor = jnp.where(upper, jnp.exp(own_total), 1.0)
    put_totals(msg, QUART, 16, own_total + got_total)
    prefix[...] = jnp.where(upper, got_total, 0.0)
    for k in range(5):
        at = pl.ds(pl.multiple_of(zq * QUART + k * 64, 64), 64)
        own_f = jnp.where(zq == 0, own_factor[k : k + 1], own_factor[k + 5 : k + 6])
        got_f = jnp.where(zq == 0, got_factor[k : k + 1], got_factor[k + 5 : k + 6])
        merged = own_f * own[at, :].astype(F32) + got_f * got[at, :].astype(F32)
        msg[k * 64 : k * 64 + 64, :] = merged.astype(BF)


def merge_kernel(bit, place, own, got, old, msg, prefix):
    zq = lax.rem(place[3], 2)
    upper = lax.rem(place[3] // bit, 2) == 1
    own_total = get_totals(own, QUART, 16)
    got_total = get_totals(got, QUART, 16)
    own_factor = jnp.where(upper, 1.0, jnp.exp(got_total))
    got_factor = jnp.where(upper, jnp.exp(own_total), 1.0)
    put_totals(msg, QUART, 16, own_total + got_total)
    prefix[...] = old[...] + jnp.where(upper, got_total, 0.0)
    for k in range(5):
        at = slice(k * 64, k * 64 + 64)
        own_f = jnp.where(zq == 0, own_factor[k : k + 1], own_factor[k + 5 : k + 6])
        got_f = jnp.where(zq == 0, got_factor[k : k + 1], got_factor[k + 5 : k + 6])
        msg[at, :] = (own_f * own[at, :].astype(F32) + got_f * got[at, :].astype(F32)).astype(BF)


def merge_side_kernel(bit, place, own, got, old, before, msg, prefix, side):
    merge_kernel(bit, place, own, got, old, msg, prefix)
    side[:QUART, :] = before[:QUART, :]
    side[QUART:, :] = got[:QUART, :]


def lines_kernel(place, r1, r2, r3, old, late, prefix):
    zq = lax.rem(place[3], 2)
    odd = lax.rem(place[2], 2) == 1
    t1 = get_totals(r1, QUART, 16)
    t2 = get_totals(r2, QUART, 16)
    t3 = get_totals(r3, QUART, 16)
    prefix[...] = old[...] + jnp.where(odd, t1, 0.0)
    late[:QUART, :] = r1[:QUART, :]
    f2 = jnp.where(odd, 1.0, jnp.exp(t3))
    f3 = jnp.where(odd, jnp.exp(t2), 1.0)
    for k in range(5):
        at = slice(k * 64, k * 64 + 64)
        a = jnp.where(zq == 0, f2[k : k + 1], f2[k + 5 : k + 6])
        b = jnp.where(zq == 0, f3[k : k + 1], f3[k + 5 : k + 6])
        late[QUART + k * 64 : QUART + k * 64 + 64, :] = (
            a * r2[at, :].astype(F32) + b * r3[at, :].astype(F32)
        ).astype(BF)


def prep_kernel(place, queries, cum_ref, lam_index, lam_table, factors, mail, levels):
    core = place[0]
    lane = lanes()
    grow = jnp.exp(cum_ref[...])
    picks = lax.broadcasted_iota(I32, (64, TOK), 0)
    onehot = (picks == lam_index[...]).astype(F32).astype(BF)

    tables = []
    for first in (0, 4):
        table = [jnp.concatenate([lam_table[:, first + i, :], jnp.zeros((12, 64), F32)], axis=0) for i in range(4)]
        table = jnp.concatenate(table, axis=0)
        hi = table.astype(BF)
        rest = table - hi.astype(F32)
        mid = rest.astype(BF)
        low = (rest - mid.astype(F32)).astype(BF)
        out = jnp.dot(hi, onehot, preferred_element_type=F32)
        out = out + jnp.dot(mid, onehot, preferred_element_type=F32)
        out = out + jnp.dot(low, onehot, preferred_element_type=F32)
        tables.append(out.T)

    def level(number):
        return pltpu.roll(tables[number // 4], (LANE - 32 * (number % 4)) % LANE, 1)

    mine = jnp.zeros((TOK, LANE), F32)
    theirs = jnp.zeros((TOK, LANE), F32)
    for number in range(5):
        value = level(3 + number) * grow
        there = (lane >= number * 16) & (lane < number * 16 + 10)
        to_first = pltpu.roll(value, number * 16, 1)
        to_second = pltpu.roll(value, (number * 16 + LANE - 10) % LANE, 1)
        mine = jnp.where(there, jnp.where(core == 0, to_first, to_second), mine)
        theirs = jnp.where(there, jnp.where(core == 0, to_second, to_first), theirs)
    factors[...] = mine
    mail[:TOK, :] = queries[...]
    hi = theirs.astype(BF)
    mail[TOK : 2 * TOK, :] = hi
    mail[2 * TOK :, :] = (theirs - hi.astype(F32)).astype(BF)

    levels[0] = level(0)
    levels[1] = level(1)
    levels[2] = jnp.where(core == 1, level(2) * grow, 0.0)


def local_kernel(side, place, queries, keys, values, cum_ref, segments, levels, skip, got, base):
    row, lane = rows(), lanes()
    cum = cum_ref[...]
    cum_t = cum.T
    near, far, zero_level = levels[0], levels[1], levels[2]
    q = queries[...]
    scores = lax.dot_general(q, keys[...], NT, preferred_element_type=F32)
    seg_row = jnp.broadcast_to(segments[...].astype(F32), (TOK, LANE))
    same = seg_row == seg_row.T
    causal = row >= lane
    for p in range(side * 5, side * 5 + 5):
        cols = slice(p * LANE, (p + 1) * LANE)
        pieces = []
        for h in (2 * p, 2 * p + 1):
            gap = jnp.where(causal, cum[:, h : h + 1] - cum_t[h : h + 1, :], -1e30)
            weight = jnp.where(same, near[:, h : h + 1], far[:, h : h + 1])
            weight = (scores * jnp.exp(gap) * weight).astype(BF)
            pieces.append(
                jnp.dot(weight, values[:, h * 64 : h * 64 + 64], preferred_element_type=F32)
            )
        read = lax.dot_general(q, got[cols, :], NT, preferred_element_type=F32)
        read = read * two_heads(zero_level[:, 2 * p : 2 * p + 1], zero_level[:, 2 * p + 1 : 2 * p + 2], lane)
        gain = two_heads(skip[:, 2 * p : 2 * p + 1], skip[:, 2 * p + 1 : 2 * p + 2], lane)
        out = slice((p % 5) * LANE, (p % 5) * LANE + LANE)
        base[:, out] = jnp.concatenate(pieces, axis=1) + read + gain * values[:, cols].astype(F32)


def level_weights(place, factors, mail, first_total, prefixes):
    core, x, z = place[0], place[2], place[3]
    lane = lanes()
    blocks = [jnp.zeros((16, LANE), F32)] + [p[...] for p in prefixes]
    blocks = blocks + [jnp.zeros((16, LANE), F32)] * (8 - len(blocks))
    chip = jnp.concatenate(blocks, axis=0).T
    first = jnp.concatenate([first_total[...]] * 8, axis=0).T
    uppers = [lax.rem(z, 2), lax.rem(z // 2, 2), lax.rem(z // 4, 2), lax.rem(x, 2), lax.rem(x // 2, 2)]
    on = jnp.zeros((TOK, LANE), F32)
    for number in range(5):
        there = (lane >= number * 16) & (lane < number * 16 + 10)
        on = jnp.where(there, uppers[number].astype(F32), on)
    own_chip = jnp.exp(chip + jnp.where(core == 1, first, 0.0)) * on
    other_chip = jnp.exp(chip + jnp.where(core == 1, 0.0, first)) * on
    other = mail[TOK : 2 * TOK, :].astype(F32) + mail[2 * TOK :, :].astype(F32)
    return factors[...] * own_chip, other * other_chip


def add_levels(numbers, place, tables, pairs, q_own, q_other, own_w, other_w, start, finish_own, finish_other):
    zq = lax.rem(place[3], 2)
    lane = lanes()
    tables = list(tables)
    for own_ref, other_ref in pairs:
        own_v, other_v = own_ref(), other_ref()
        tables.append(
            jnp.concatenate(
                [jnp.where(zq == 0, own_v, other_v), jnp.where(zq == 0, other_v, own_v)], axis=0
            )
        )
    for p in range(5):
        cols = slice(p * LANE, (p + 1) * LANE)
        acc_own, acc_other = start(cols)
        for number, table in zip(numbers, tables):
            a, b = number * 16 + 2 * p, number * 16 + 2 * p + 1
            piece = table[p * LANE : (p + 1) * LANE]
            read = lax.dot_general(q_own, piece, NT, preferred_element_type=F32)
            acc_own = acc_own + read * two_heads(own_w[:, a : a + 1], own_w[:, b : b + 1], lane)
            read = lax.dot_general(q_other, piece, NT, preferred_element_type=F32)
            acc_other = acc_other + read * two_heads(other_w[:, a : a + 1], other_w[:, b : b + 1], lane)
        finish_own(cols, acc_own)
        finish_other(cols, acc_other)


def rows_of(ref, start=0):
    return lambda: ref[start : start + QUART, :]


def cross_kernel(
    place, queries, factors, mail, first_total, p2, p3, p4, p5, got1, got2, got3, side, own, other, own_w, other_w
):
    mine, theirs = level_weights(place, factors, mail, first_total, [p2, p3, p4, p5])
    own_w[...] = mine
    other_w[...] = theirs
    zero = jnp.zeros((TOK, LANE), F32)

    def keep_own(cols, value):
        own[:, cols] = value

    def keep_other(cols, value):
        other[:, cols] = value

    pairs = [(rows_of(got2), rows_of(side)), (rows_of(got3), rows_of(side, QUART))]
    add_levels(
        (0, 1, 2), place, [got1[:HALF, :]], pairs, queries[...], mail[:TOK, :], mine, theirs,
        lambda cols: (zero, zero), keep_own, keep_other,
    )


def late_kernel(place, queries, mail, own_w, other_w, late, late_side, own_in, other_in, own, back):
    def keep_own(cols, value):
        own[:, cols] = value

    def keep_back(cols, value):
        back[:, cols] = value.astype(BF)

    pairs = [
        (rows_of(late), rows_of(late_side)),
        (rows_of(late, QUART), rows_of(late_side, QUART)),
    ]
    add_levels(
        (3, 4), place, [], pairs, queries[...], mail[:TOK, :], own_w[...], other_w[...],
        lambda cols: (own_in[:, cols], other_in[:, cols]), keep_own, keep_back,
    )


def project_blocks(place, y_ref, w_refs, out_refs):
    core, y = place[0], place[1]
    y_mine = y_ref[:, pl.ds(pl.multiple_of(core * HALF, HALF), HALF)]
    y_rest = y_ref[:, pl.ds(pl.multiple_of((1 - core) * HALF, HALF), HALF)]
    count = len(w_refs) // 4
    for block in range(count):
        mine_w = jnp.concatenate([w_refs[2 * block][...], w_refs[2 * block + 1][...]], axis=0)
        at = 2 * (count + block)
        rest_w = jnp.concatenate([w_refs[at][...], w_refs[at + 1][...]], axis=0)
        total = lax.dot_general(y_mine, mine_w, NT, preferred_element_type=F32)
        total = total + lax.dot_general(y_rest, rest_w, NT, preferred_element_type=F32)
        store(y, out_refs, slice(block * HALF, (block + 1) * HALF), total.astype(BF))


def store(y, out_refs, cols, value):
    part = TOK // NY
    for d in range(NY):
        for owner in range(NY):

            @pl.when((y ^ d) == owner)
            def _():
                out_refs[d][:, cols] = value[owner * part : (owner + 1) * part]


def first_kernel(place, low, high, own, back, gate, gain, *refs):
    core, y = place[0], place[1]
    w_refs, y_ref, out_refs = refs[:8], refs[8], refs[9:]
    lane = lanes()
    squares = jnp.zeros((TOK, LANE), F32)
    for p in range(10):
        cols = slice(p * LANE, (p + 1) * LANE)
        inner = slice((p % 5) * LANE, (p % 5) * LANE + LANE)
        cross = jnp.where(core == p // 5, own[:, inner], back[:, inner].astype(F32))
        gated = (low if p < 5 else high)[:, inner] + cross
        v = gate[:, cols].astype(F32)
        gated = gated * (v / (1.0 + jnp.exp(-v)))
        squares = squares + gated * gated
        y_ref[:, cols] = (gated * gain[p : p + 1, :]).astype(BF)
    squares = jnp.sum(squares, axis=1, keepdims=True)
    hi = squares.astype(BF).astype(F32)
    mid = (squares - hi).astype(BF).astype(F32)
    low = squares - hi - mid
    squares = jnp.where(lane == 0, hi, jnp.where(lane == 1, mid, jnp.where(lane == 2, low, 0.0)))
    store(y, out_refs, slice(2 * HALF, 2 * HALF + LANE), squares.astype(BF))
    project_blocks(place, y_ref, w_refs, out_refs)


def second_kernel(place, y_ref, *refs):
    project_blocks(place, y_ref, refs[:8], refs[8:])


def finish_kernel(place, *refs):
    x, z = place[2], place[3]
    firsts, seconds, out_ref = refs[:4], refs[4:8], refs[8]

    def total(parts, cols):
        left = parts[0][:, cols].astype(F32) + parts[1][:, cols].astype(F32)
        return left + (parts[2][:, cols].astype(F32) + parts[3][:, cols].astype(F32))

    squares = total(firsts, slice(2 * HALF, 2 * HALF + LANE))
    squares = squares[:, 0:1] + squares[:, 1:2] + squares[:, 2:3]
    inv = lax.rsqrt(squares / DI + EPS)
    amount = lax.rem(z + (NZ - 2), NZ) * 80
    for block in range(4):
        parts = firsts if block < 2 else seconds
        part = total(parts, slice((block % 2) * HALF, (block % 2 + 1) * HALF)) * inv
        part = pltpu.roll(part, amount, 1)
        at = pl.multiple_of((x ^ block) * HALF, HALF)
        out_ref[:, pl.ds(at, HALF)] = part.astype(BF)


def gather_weights(out_proj):
    core = lax.axis_index("core")
    own_rows = out_proj.T
    other_rows = flip(own_rows, "core", 1, 2)
    first = core == 0
    pair = jnp.concatenate(
        [jnp.where(first, own_rows, other_rows), jnp.where(first, other_rows, own_rows)], axis=0
    )
    mine = lax.dynamic_slice_in_dim(pair, core * HALF, HALF, 1)
    below1 = shift(mine, "z", 1, NZ)
    above1 = shift(mine, "z", -1, NZ)
    below2 = shift(below1, "z", 1, NZ)
    above2 = shift(above1, "z", -1, NZ)
    below3 = shift(below2, "z", 1, NZ)
    above3 = shift(above2, "z", -1, NZ)
    above4 = shift(above3, "z", -1, NZ)
    near = joined(below2, below1, mine, above1)
    far = joined(above2, above3, above4, below3)
    near_1 = flip(near, "x", 1, NX)
    near_3 = flip(near, "x", 3, NX)
    far_1 = flip(far, "x", 1, NX)
    far_3 = flip(far, "x", 3, NX)
    near_2 = flip(near_3, "x", 1, NX)
    far_2 = flip(far_1, "x", 3, NX)
    own = [near, far, near_1, far_1, near_2, far_2, near_3, far_3]
    order = (0, 1, 2, 6, 4, 3, 7, 5)
    others = [None] * 8
    for at in order:
        others[at] = flip(own[at], "core", 1, 2)
    return own, others


def join_kernel(place, a, b, c, d, out):
    for number, ref in enumerate((a, b, c, d)):
        out[number * 80 : (number + 1) * 80, :] = ref[...]


def joined(*pieces):
    return call(join_kernel, jnp.zeros((1,), I32), pieces, [shaped(QUART, HALF)], flops=10**6)[0]


def mixer(
    queries, key_rows, values, gate_rows, log_decay, skip_gain, lam_index, segments, lam_table, norm_gain, out_proj
):
    places = [lax.axis_index(name) for name in ("core", "y", "x", "z")]
    place = jnp.stack(places).astype(I32)
    own_w, other_w = gather_weights(out_proj)
    state, cum = call(
        state_kernel, place, (values, key_rows, log_decay.T),
        [shaped(COLS + 96, NST), shaped(TOK, LANE, dtype=F32)],
        vmem=6,
    )
    got0 = flip(state, "core", 1, 2)
    quart = shaped(QUART + 48, NST)
    line = shaped(16, LANE, dtype=F32)
    msg1, first_total = call(pair_kernel, place, (state, got0), [shaped(HALF + 48, NST), line])
    got1 = flip(msg1, "z", 1, NZ)
    msg2, p2 = call(chip_kernel, place, (msg1, got1), [quart, line])
    got2 = flip(msg2, "z", 2, NZ)
    msg3, p3 = call(lambda *r: merge_kernel(2, *r), place, (msg2, got2, p2), [quart, line])
    got3 = flip(msg3, "z", 6, NZ)
    msg4, p4, side = call(
        lambda *r: merge_side_kernel(4, *r), place, (msg3, got3, p3, got2), [quart, line, shaped(HALF, NST)]
    )
    r1 = flip(msg4, "x", 1, NX)
    r3 = flip(msg4, "x", 3, NX)
    r2 = flip(msg4, "x", 2, NX)
    side = flip(side, "z", 1, NZ)

    half = shaped(TOK, HALF, dtype=F32)
    factors, mail, levels = call(
        prep_kernel, place,
        (queries, cum, lam_index.reshape(1, TOK), lam_table.transpose(2, 1, 0)),
        [shaped(TOK, LANE, dtype=F32), shaped(3 * TOK, LANE), shaped(3, TOK, LANE, dtype=F32)],
    )
    bases = [
        call(
            lambda *r, side=side: local_kernel(side, *r), place,
            (queries, key_rows, values, cum, segments.reshape(1, TOK), levels, skip_gain.reshape(1, HEADS), got0),
            [half],
            vmem=6,
        )[0]
        for side in range(2)
    ]
    mail = flip(mail, "core", 1, 2)
    late, p5 = call(lines_kernel, place, (r1, r2, r3, p4), [shaped(HALF, NST), line])
    late_side = flip(late, "z", 1, NZ)
    square = shaped(TOK, LANE, dtype=F32)
    own_acc, other_acc, own_lw, other_lw = call(
        cross_kernel, place,
        (queries, factors, mail, first_total, p2, p3, p4, p5, got1, got2, got3, side),
        [half, half, square, square],
        vmem=8,
    )
    own_cross, back = call(
        late_kernel, place,
        (queries, mail, own_lw, other_lw, late, late_side, own_acc, other_acc),
        [half, shaped(TOK, HALF)],
        vmem=8,
    )
    back = flip(back, "core", 1, 2)
    part = TOK // NY
    scaled, *firsts = call(
        first_kernel, place,
        (*bases, own_cross, back, gate_rows, norm_gain.reshape(10, LANE), *own_w[:4], *other_w[:4]),
        [shaped(TOK, COLS)] + [shaped(part, 2 * HALF + LANE)] * NY,
        flops=5 * 10**8,
        vmem=12,
    )
    seconds = call(
        second_kernel, place, (scaled, *own_w[4:], *other_w[4:]),
        [shaped(part, 2 * HALF)] * NY,
        flops=5 * 10**8,
        vmem=12,
    )
    arrived = []
    for parts in (firsts, seconds):
        arrived.append(parts[0])
        for d in (2, 1, 3):
            arrived.append(flip(parts[d], "y", d, NY))
    return call(finish_kernel, place, arrived, [shaped(part, 2560)])[0]


def solution(mesh):
    inner = Mesh(mesh.devices.reshape(NX, NZ, 2, NY), ("x", "z", "core", "y"))
    seq = ("x", "z", "core")
    return jax.shard_map(
        mixer,
        mesh=inner,
        in_specs=(
            P(seq, None),
            P(seq, None),
            P(seq, "y"),
            P(seq, "y"),
            P(seq, "y"),
            P("y"),
            P(seq),
            P(seq),
            P(None, None, "y"),
            P("y"),
            P("y", seq),
        ),
        out_specs=P((*seq, "y"), None),
        check_vma=False,
    )
```

```python
import jax
import jax.numpy as jnp
from jax import lax
from jax.experimental import pallas as pl
from jax.experimental.pallas import tpu as pltpu
from jax.sharding import Mesh
from jax.sharding import PartitionSpec as P

DI = 5120
EPS = 1e-05
NX, NZ, NY = 4, 8, 4
TOK, COLS, HEADS, NST = 128, 1280, 20, 128
HALF, QUART = 640, 320
LANE = 128
BF = jnp.bfloat16
F32 = jnp.float32
I32 = jnp.int32
NT = (((1,), (1,)), ((), ()))
TN = (((0,), (0,)), ((), ()))


def flip(value, axis, mask, size):
    return lax.ppermute(value, axis, [(i, i ^ mask) for i in range(size)])


def shift(value, axis, step, size):
    return lax.ppermute(value, axis, [(i, (i + step) % size) for i in range(size)])


def call(body, place, args, outs, scratch=(), flops=10**8, vmem=4):
    return pl.pallas_call(
        body,
        out_shape=outs,
        in_specs=[pl.BlockSpec(memory_space=pltpu.SMEM)]
        + [pl.BlockSpec(memory_space=pltpu.VMEM)] * len(args),
        out_specs=[pl.BlockSpec(memory_space=pltpu.VMEM)] * len(outs),
        scratch_shapes=list(scratch),
        compiler_params=pltpu.CompilerParams(vmem_limit_bytes=vmem << 20),
        cost_estimate=pl.CostEstimate(flops=flops, bytes_accessed=1 << 20, transcendentals=0),
    )(place, *args)


def shaped(*shape, dtype=BF):
    return jax.ShapeDtypeStruct(shape, dtype)


def lanes():
    return lax.broadcasted_iota(I32, (TOK, LANE), 1)


def rows():
    return lax.broadcasted_iota(I32, (TOK, LANE), 0)


def two_heads(first, second, lane):
    return jnp.where(lane < 64, first, second)


def put_totals(ref, at, size, totals):
    hi = totals.astype(BF)
    rest = totals - hi.astype(F32)
    mid = rest.astype(BF)
    low = (rest - mid.astype(F32)).astype(BF)
    ref[at : at + size, :] = hi
    ref[at + size : at + 2 * size, :] = mid
    ref[at + 2 * size : at + 3 * size, :] = low


def get_totals(ref, at, size):
    parts = ref[at : at + 3 * size, :].astype(F32)
    return parts[:size] + parts[size : 2 * size] + parts[2 * size :]


def state_kernel(place, values, keys, log_decay, msg, cum_ref):
    lane = lanes()
    cum = jnp.concatenate([log_decay[...], jnp.zeros((4, TOK), F32)], axis=0)
    step = 1
    while step < TOK:
        cum = cum + jnp.where(lane[:24] >= step, pltpu.roll(cum, step, 1), 0.0)
        step *= 2
    cum = jnp.concatenate([cum, jnp.zeros((TOK - 24, TOK), F32)], axis=0).T
    cum_ref[...] = cum
    total = cum[TOK - 1 : TOK, :]
    factor = jnp.exp(total - cum)
    spread = jnp.broadcast_to(total, (TOK, LANE))
    spread = jnp.where(lane < 10, spread, pltpu.roll(spread, 6, 1))
    spread = jnp.where((lane < 10) | ((lane >= 16) & (lane < 26)), spread, 0.0)
    put_totals(msg, COLS, 32, spread.T[:32])
    key = keys[...]
    for p in range(10):
        cols = slice(p * LANE, (p + 1) * LANE)
        wide = two_heads(factor[:, 2 * p : 2 * p + 1], factor[:, 2 * p + 1 : 2 * p + 2], lane)
        decayed = (values[:, cols].astype(F32) * wide).astype(BF)
        msg[cols, :] = lax.dot_general(decayed, key, TN, preferred_element_type=F32).astype(BF)


def pair_kernel(place, own, got, msg, prefix):
    core = place[0]
    own_total = get_totals(own, COLS, 32)
    got_total = get_totals(got, COLS, 32)
    own_total = jnp.where(core == 0, own_total[:16], own_total[16:])
    got_total = jnp.where(core == 0, got_total[:16], got_total[16:])
    upper = core == 1
    own_factor = jnp.where(upper, 1.0, jnp.exp(got_total))
    got_factor = jnp.where(upper, jnp.exp(own_total), 1.0)
    put_totals(msg, HALF, 16, own_total + got_total)
    prefix[...] = jnp.where(upper, got_total, own_total)
    for h in range(10):
        at = pl.ds(pl.multiple_of(core * HALF + h * 64, 64), 64)
        merged = own_factor[h : h + 1] * own[at, :].astype(F32) + got_factor[h : h + 1] * got[at, :].astype(F32)
        msg[h * 64 : h * 64 + 64, :] = merged.astype(BF)


def chip_kernel(place, own, got, msg, prefix):
    zq = lax.rem(place[3], 2)
    upper = zq == 1
    own_total = get_totals(own, HALF, 16)
    got_total = get_totals(got, HALF, 16)
    own_factor = jnp.where(upper, 1.0, jnp.exp(got_total))
    got_factor = jnp.where(upper, jnp.exp(own_total), 1.0)
    put_totals(msg, QUART, 16, own_total + got_total)
    prefix[...] = jnp.where(upper, got_total, 0.0)
    for k in range(5):
        at = pl.ds(pl.multiple_of(zq * QUART + k * 64, 64), 64)
        own_f = jnp.where(zq == 0, own_factor[k : k + 1], own_factor[k + 5 : k + 6])
        got_f = jnp.where(zq == 0, got_factor[k : k + 1], got_factor[k + 5 : k + 6])
        merged = own_f * own[at, :].astype(F32) + got_f * got[at, :].astype(F32)
        msg[k * 64 : k * 64 + 64, :] = merged.astype(BF)


def merge_kernel(bit, place, own, got, old, msg, prefix):
    zq = lax.rem(place[3], 2)
    upper = lax.rem(place[3] // bit, 2) == 1
    own_total = get_totals(own, QUART, 16)
    got_total = get_totals(got, QUART, 16)
    own_factor = jnp.where(upper, 1.0, jnp.exp(got_total))
    got_factor = jnp.where(upper, jnp.exp(own_total), 1.0)
    put_totals(msg, QUART, 16, own_total + got_total)
    prefix[...] = old[...] + jnp.where(upper, got_total, 0.0)
    for k in range(5):
        at = slice(k * 64, k * 64 + 64)
        own_f = jnp.where(zq == 0, own_factor[k : k + 1], own_factor[k + 5 : k + 6])
        got_f = jnp.where(zq == 0, got_factor[k : k + 1], got_factor[k + 5 : k + 6])
        msg[at, :] = (own_f * own[at, :].astype(F32) + got_f * got[at, :].astype(F32)).astype(BF)


def merge_side_kernel(bit, place, own, got, old, before, msg, prefix, side):
    merge_kernel(bit, place, own, got, old, msg, prefix)
    side[:QUART, :] = before[:QUART, :]
    side[QUART:, :] = got[:QUART, :]


def lines_kernel(place, r1, r2, r3, old, late, prefix):
    zq = lax.rem(place[3], 2)
    odd = lax.rem(place[2], 2) == 1
    t1 = get_totals(r1, QUART, 16)
    t2 = get_totals(r2, QUART, 16)
    t3 = get_totals(r3, QUART, 16)
    prefix[...] = old[...] + jnp.where(odd, t1, 0.0)
    late[:QUART, :] = r1[:QUART, :]
    f2 = jnp.where(odd, 1.0, jnp.exp(t3))
    f3 = jnp.where(odd, jnp.exp(t2), 1.0)
    for k in range(5):
        at = slice(k * 64, k * 64 + 64)
        a = jnp.where(zq == 0, f2[k : k + 1], f2[k + 5 : k + 6])
        b = jnp.where(zq == 0, f3[k : k + 1], f3[k + 5 : k + 6])
        late[QUART + k * 64 : QUART + k * 64 + 64, :] = (
            a * r2[at, :].astype(F32) + b * r3[at, :].astype(F32)
        ).astype(BF)


def prep_kernel(place, queries, cum_ref, lam_index, lam_table, factors, mail, levels):
    core = place[0]
    lane = lanes()
    grow = jnp.exp(cum_ref[...])
    picks = lax.broadcasted_iota(I32, (64, TOK), 0)
    onehot = (picks == lam_index[...]).astype(F32).astype(BF)

    tables = []
    for first in (0, 4):
        table = [jnp.concatenate([lam_table[:, first + i, :], jnp.zeros((12, 64), F32)], axis=0) for i in range(4)]
        table = jnp.concatenate(table, axis=0)
        hi = table.astype(BF)
        rest = table - hi.astype(F32)
        mid = rest.astype(BF)
        low = (rest - mid.astype(F32)).astype(BF)
        out = jnp.dot(hi, onehot, preferred_element_type=F32)
        out = out + jnp.dot(mid, onehot, preferred_element_type=F32)
        out = out + jnp.dot(low, onehot, preferred_element_type=F32)
        tables.append(out.T)

    def level(number):
        return pltpu.roll(tables[number // 4], (LANE - 32 * (number % 4)) % LANE, 1)

    mine = jnp.zeros((TOK, LANE), F32)
    theirs = jnp.zeros((TOK, LANE), F32)
    for number in range(5):
        value = level(3 + number) * grow
        there = (lane >= number * 16) & (lane < number * 16 + 10)
        to_first = pltpu.roll(value, number * 16, 1)
        to_second = pltpu.roll(value, (number * 16 + LANE - 10) % LANE, 1)
        mine = jnp.where(there, jnp.where(core == 0, to_first, to_second), mine)
        theirs = jnp.where(there, jnp.where(core == 0, to_second, to_first), theirs)
    factors[...] = mine
    mail[:TOK, :] = queries[...]
    hi = theirs.astype(BF)
    mail[TOK : 2 * TOK, :] = hi
    mail[2 * TOK :, :] = (theirs - hi.astype(F32)).astype(BF)

    levels[0] = level(0)
    levels[1] = level(1)
    levels[2] = jnp.where(core == 1, level(2) * grow, 0.0)


def local_kernel(side, place, queries, keys, values, cum_ref, segments, levels, skip, got, base):
    row, lane = rows(), lanes()
    cum = cum_ref[...]
    cum_t = cum.T
    near, far, zero_level = levels[0], levels[1], levels[2]
    q = queries[...]
    scores = lax.dot_general(q, keys[...], NT, preferred_element_type=F32)
    seg_row = jnp.broadcast_to(segments[...].astype(F32), (TOK, LANE))
    same = seg_row == seg_row.T
    causal = row >= lane
    for p in range(side * 5, side * 5 + 5):
        cols = slice(p * LANE, (p + 1) * LANE)
        pieces = []
        for h in (2 * p, 2 * p + 1):
            gap = jnp.where(causal, cum[:, h : h + 1] - cum_t[h : h + 1, :], -1e30)
            weight = jnp.where(same, near[:, h : h + 1], far[:, h : h + 1])
            weight = (scores * jnp.exp(gap) * weight).astype(BF)
            pieces.append(
                jnp.dot(weight, values[:, h * 64 : h * 64 + 64], preferred_element_type=F32)
            )
        read = lax.dot_general(q, got[cols, :], NT, preferred_element_type=F32)
        read = read * two_heads(zero_level[:, 2 * p : 2 * p + 1], zero_level[:, 2 * p + 1 : 2 * p + 2], lane)
        gain = two_heads(skip[:, 2 * p : 2 * p + 1], skip[:, 2 * p + 1 : 2 * p + 2], lane)
        out = slice((p % 5) * LANE, (p % 5) * LANE + LANE)
        base[:, out] = jnp.concatenate(pieces, axis=1) + read + gain * values[:, cols].astype(F32)


def level_weights(place, factors, mail, first_total, prefixes):
    core, x, z = place[0], place[2], place[3]
    lane = lanes()
    blocks = [jnp.zeros((16, LANE), F32)] + [p[...] for p in prefixes]
    blocks = blocks + [jnp.zeros((16, LANE), F32)] * (8 - len(blocks))
    chip = jnp.concatenate(blocks, axis=0).T
    first = jnp.concatenate([first_total[...]] * 8, axis=0).T
    uppers = [lax.rem(z, 2), lax.rem(z // 2, 2), lax.rem(z // 4, 2), lax.rem(x, 2), lax.rem(x // 2, 2)]
    on = jnp.zeros((TOK, LANE), F32)
    for number in range(5):
        there = (lane >= number * 16) & (lane < number * 16 + 10)
        on = jnp.where(there, uppers[number].astype(F32), on)
    own_chip = jnp.exp(chip + jnp.where(core == 1, first, 0.0)) * on
    other_chip = jnp.exp(chip + jnp.where(core == 1, 0.0, first)) * on
    other = mail[TOK : 2 * TOK, :].astype(F32) + mail[2 * TOK :, :].astype(F32)
    return factors[...] * own_chip, other * other_chip


def add_levels(numbers, place, tables, pairs, q_own, q_other, own_w, other_w, start, finish_own, finish_other):
    zq = lax.rem(place[3], 2)
    lane = lanes()
    tables = list(tables)
    for own_ref, other_ref in pairs:
        own_v, other_v = own_ref(), other_ref()
        tables.append(
            jnp.concatenate(
                [jnp.where(zq == 0, own_v, other_v), jnp.where(zq == 0, other_v, own_v)], axis=0
            )
        )
    for p in range(5):
        cols = slice(p * LANE, (p + 1) * LANE)
        acc_own, acc_other = start(cols)
        for number, table in zip(numbers, tables):
            a, b = number * 16 + 2 * p, number * 16 + 2 * p + 1
            piece = table[p * LANE : (p + 1) * LANE]
            read = lax.dot_general(q_own, piece, NT, preferred_element_type=F32)
            acc_own = acc_own + read * two_heads(own_w[:, a : a + 1], own_w[:, b : b + 1], lane)
            read = lax.dot_general(q_other, piece, NT, preferred_element_type=F32)
            acc_other = acc_other + read * two_heads(other_w[:, a : a + 1], other_w[:, b : b + 1], lane)
        finish_own(cols, acc_own)
        finish_other(cols, acc_other)


def rows_of(ref, start=0):
    return lambda: ref[start : start + QUART, :]


def cross_kernel(
    place, queries, factors, mail, first_total, p2, p3, p4, p5, got1, got2, got3, side, own, other, own_w, other_w
):
    mine, theirs = level_weights(place, factors, mail, first_total, [p2, p3, p4, p5])
    own_w[...] = mine
    other_w[...] = theirs
    zero = jnp.zeros((TOK, LANE), F32)

    def keep_own(cols, value):
        own[:, cols] = value

    def keep_other(cols, value):
        other[:, cols] = value

    pairs = [(rows_of(got2), rows_of(side)), (rows_of(got3), rows_of(side, QUART))]
    add_levels(
        (0, 1, 2), place, [got1[:HALF, :]], pairs, queries[...], mail[:TOK, :], mine, theirs,
        lambda cols: (zero, zero), keep_own, keep_other,
    )


def late_kernel(place, queries, mail, own_w, other_w, late, late_side, own_in, other_in, own, back):
    def keep_own(cols, value):
        own[:, cols] = value

    def keep_back(cols, value):
        back[:, cols] = value.astype(BF)

    pairs = [
        (rows_of(late), rows_of(late_side)),
        (rows_of(late, QUART), rows_of(late_side, QUART)),
    ]
    add_levels(
        (3, 4), place, [], pairs, queries[...], mail[:TOK, :], own_w[...], other_w[...],
        lambda cols: (own_in[:, cols], other_in[:, cols]), keep_own, keep_back,
    )


def project_kernel(place, low, high, own, back, gate, gain, *refs):
    core, y = place[0], place[1]
    w_refs, out_refs, y_ref = refs[:16], refs[16:20], refs[20]
    part = TOK // NY
    lane = lanes()
    squares = jnp.zeros((TOK, LANE), F32)
    for p in range(10):
        cols = slice(p * LANE, (p + 1) * LANE)
        inner = slice((p % 5) * LANE, (p % 5) * LANE + LANE)
        cross = jnp.where(core == p // 5, own[:, inner], back[:, inner].astype(F32))
        gated = (low if p < 5 else high)[:, inner] + cross
        v = gate[:, cols].astype(F32)
        gated = gated * (v / (1.0 + jnp.exp(-v)))
        squares = squares + gated * gated
        y_ref[:, cols] = (gated * gain[p : p + 1, :]).astype(BF)
    squares = jnp.sum(squares, axis=1, keepdims=True)
    hi = squares.astype(BF).astype(F32)
    mid = (squares - hi).astype(BF).astype(F32)
    low = squares - hi - mid
    squares = jnp.where(lane == 0, hi, jnp.where(lane == 1, mid, jnp.where(lane == 2, low, 0.0)))
    squares = squares.astype(BF)
    mine = pl.ds(pl.multiple_of(core * HALF, HALF), HALF)
    rest = pl.ds(pl.multiple_of((1 - core) * HALF, HALF), HALF)
    y_mine, y_rest = y_ref[:, mine], y_ref[:, rest]

    def store(d, cols, value):
        for owner in range(NY):

            @pl.when((y ^ d) == owner)
            def _():
                out_refs[d][:, cols] = value[owner * part : (owner + 1) * part]

    for d in range(NY):
        store(d, slice(2560, 2688), squares)
    for block in range(4):
        mine_w = jnp.concatenate([w_refs[2 * block][...], w_refs[2 * block + 1][...]], axis=0)
        rest_w = jnp.concatenate([w_refs[8 + 2 * block][...], w_refs[9 + 2 * block][...]], axis=0)
        total = lax.dot_general(y_mine, mine_w, NT, preferred_element_type=F32)
        total = total + lax.dot_general(y_rest, rest_w, NT, preferred_element_type=F32)
        total = total.astype(BF)
        for d in range(NY):
            store(d, slice(block * HALF, (block + 1) * HALF), total)


def finish_kernel(place, a_ref, b_ref, c_ref, d_ref, out_ref):
    x, z = place[2], place[3]

    def total(cols):
        left = a_ref[:, cols].astype(F32) + b_ref[:, cols].astype(F32)
        return left + (c_ref[:, cols].astype(F32) + d_ref[:, cols].astype(F32))

    squares = total(slice(2560, 2688))
    squares = squares[:, 0:1] + squares[:, 1:2] + squares[:, 2:3]
    inv = lax.rsqrt(squares / DI + EPS)
    amount = lax.rem(z + (NZ - 2), NZ) * 80
    for block in range(4):
        part = total(slice(block * HALF, (block + 1) * HALF)) * inv
        part = pltpu.roll(part, amount, 1)
        at = pl.multiple_of((x ^ block) * HALF, HALF)
        out_ref[:, pl.ds(at, HALF)] = part.astype(BF)


def gather_weights(out_proj):
    core = lax.axis_index("core")
    own_rows = out_proj.T
    other_rows = flip(own_rows, "core", 1, 2)
    first = core == 0
    pair = jnp.concatenate(
        [jnp.where(first, own_rows, other_rows), jnp.where(first, other_rows, own_rows)], axis=0
    )
    mine = lax.dynamic_slice_in_dim(pair, core * HALF, HALF, 1)
    below1 = shift(mine, "z", 1, NZ)
    above1 = shift(mine, "z", -1, NZ)
    below2 = shift(below1, "z", 1, NZ)
    above2 = shift(above1, "z", -1, NZ)
    below3 = shift(below2, "z", 1, NZ)
    above3 = shift(above2, "z", -1, NZ)
    above4 = shift(above3, "z", -1, NZ)
    near = joined(below2, below1, mine, above1)
    far = joined(above2, above3, above4, below3)
    near_1 = flip(near, "x", 1, NX)
    near_3 = flip(near, "x", 3, NX)
    far_1 = flip(far, "x", 1, NX)
    far_3 = flip(far, "x", 3, NX)
    near_2 = flip(near_3, "x", 1, NX)
    far_2 = flip(far_1, "x", 3, NX)
    own = [near, far, near_1, far_1, near_2, far_2, near_3, far_3]
    order = (0, 1, 2, 6, 4, 3, 7, 5)
    others = [None] * 8
    for at in order:
        others[at] = flip(own[at], "core", 1, 2)
    return own, others


def join_kernel(place, a, b, c, d, out):
    for number, ref in enumerate((a, b, c, d)):
        out[number * 80 : (number + 1) * 80, :] = ref[...]


def joined(*pieces):
    return call(join_kernel, jnp.zeros((1,), I32), pieces, [shaped(QUART, HALF)], flops=10**6)[0]


def mixer(
    queries, key_rows, values, gate_rows, log_decay, skip_gain, lam_index, segments, lam_table, norm_gain, out_proj
):
    places = [lax.axis_index(name) for name in ("core", "y", "x", "z")]
    place = jnp.stack(places).astype(I32)
    own_w, other_w = gather_weights(out_proj)
    state, cum = call(
        state_kernel, place, (values, key_rows, log_decay.T),
        [shaped(COLS + 96, NST), shaped(TOK, LANE, dtype=F32)],
        vmem=6,
    )
    got0 = flip(state, "core", 1, 2)
    quart = shaped(QUART + 48, NST)
    line = shaped(16, LANE, dtype=F32)
    msg1, first_total = call(pair_kernel, place, (state, got0), [shaped(HALF + 48, NST), line])
    got1 = flip(msg1, "z", 1, NZ)
    msg2, p2 = call(chip_kernel, place, (msg1, got1), [quart, line])
    got2 = flip(msg2, "z", 2, NZ)
    msg3, p3 = call(lambda *r: merge_kernel(2, *r), place, (msg2, got2, p2), [quart, line])
    got3 = flip(msg3, "z", 6, NZ)
    msg4, p4, side = call(
        lambda *r: merge_side_kernel(4, *r), place, (msg3, got3, p3, got2), [quart, line, shaped(HALF, NST)]
    )
    r1 = flip(msg4, "x", 1, NX)
    r3 = flip(msg4, "x", 3, NX)
    r2 = flip(msg4, "x", 2, NX)
    side = flip(side, "z", 1, NZ)

    half = shaped(TOK, HALF, dtype=F32)
    factors, mail, levels = call(
        prep_kernel, place,
        (queries, cum, lam_index.reshape(1, TOK), lam_table.transpose(2, 1, 0)),
        [shaped(TOK, LANE, dtype=F32), shaped(3 * TOK, LANE), shaped(3, TOK, LANE, dtype=F32)],
    )
    bases = [
        call(
            lambda *r, side=side: local_kernel(side, *r), place,
            (queries, key_rows, values, cum, segments.reshape(1, TOK), levels, skip_gain.reshape(1, HEADS), got0),
            [half],
            vmem=6,
        )[0]
        for side in range(2)
    ]
    mail = flip(mail, "core", 1, 2)
    late, p5 = call(lines_kernel, place, (r1, r2, r3, p4), [shaped(HALF, NST), line])
    late_side = flip(late, "z", 1, NZ)
    square = shaped(TOK, LANE, dtype=F32)
    own_acc, other_acc, own_lw, other_lw = call(
        cross_kernel, place,
        (queries, factors, mail, first_total, p2, p3, p4, p5, got1, got2, got3, side),
        [half, half, square, square],
        vmem=8,
    )
    own_cross, back = call(
        late_kernel, place,
        (queries, mail, own_lw, other_lw, late, late_side, own_acc, other_acc),
        [half, shaped(TOK, HALF)],
        vmem=8,
    )
    back = flip(back, "core", 1, 2)
    parts = call(
        project_kernel, place,
        (*bases, own_cross, back, gate_rows, norm_gain.reshape(10, LANE), *own_w, *other_w),
        [shaped(TOK // NY, 2688)] * NY,
        scratch=[pltpu.VMEM((TOK, COLS), BF)],
        flops=10**9,
        vmem=24,
    )
    arrived = [parts[0]]
    for d in (2, 1, 3):
        arrived.append(flip(parts[d], "y", d, NY))
    return call(finish_kernel, place, arrived, [shaped(TOK // NY, 2560)])[0]


def solution(mesh):
    inner = Mesh(mesh.devices.reshape(NX, NZ, 2, NY), ("x", "z", "core", "y"))
    seq = ("x", "z", "core")
    return jax.shard_map(
        mixer,
        mesh=inner,
        in_specs=(
            P(seq, None),
            P(seq, None),
            P(seq, "y"),
            P(seq, "y"),
            P(seq, "y"),
            P("y"),
            P(seq),
            P(seq),
            P(None, None, "y"),
            P("y"),
            P("y", seq),
        ),
        out_specs=P((*seq, "y"), None),
        check_vma=False,
    )
```

```python
import jax
import jax.numpy as jnp
from jax import lax
from jax.experimental import pallas as pl
from jax.experimental.pallas import tpu as pltpu
from jax.sharding import Mesh
from jax.sharding import PartitionSpec as P

DI = 5120
EPS = 1e-05
NX, NZ, NY = 4, 8, 4
TOK, COLS, HEADS, NST = 128, 1280, 20, 128
HALF, QUART = 640, 320
LANE = 128
BF = jnp.bfloat16
F32 = jnp.float32
I32 = jnp.int32
NT = (((1,), (1,)), ((), ()))
TN = (((0,), (0,)), ((), ()))


def flip(value, axis, mask, size):
    return lax.ppermute(value, axis, [(i, i ^ mask) for i in range(size)])


def shift(value, axis, step, size):
    return lax.ppermute(value, axis, [(i, (i + step) % size) for i in range(size)])


def call(body, place, args, outs, scratch=(), flops=10**8, vmem=4):
    return pl.pallas_call(
        body,
        out_shape=outs,
        in_specs=[pl.BlockSpec(memory_space=pltpu.SMEM)]
        + [pl.BlockSpec(memory_space=pltpu.VMEM)] * len(args),
        out_specs=[pl.BlockSpec(memory_space=pltpu.VMEM)] * len(outs),
        scratch_shapes=list(scratch),
        compiler_params=pltpu.CompilerParams(vmem_limit_bytes=vmem << 20),
        cost_estimate=pl.CostEstimate(flops=flops, bytes_accessed=1 << 20, transcendentals=0),
    )(place, *args)


def shaped(*shape, dtype=BF):
    return jax.ShapeDtypeStruct(shape, dtype)


def lanes():
    return lax.broadcasted_iota(I32, (TOK, LANE), 1)


def rows():
    return lax.broadcasted_iota(I32, (TOK, LANE), 0)


def two_heads(first, second, lane):
    return jnp.where(lane < 64, first, second)


def put_totals(ref, at, size, totals):
    hi = totals.astype(BF)
    rest = totals - hi.astype(F32)
    mid = rest.astype(BF)
    low = (rest - mid.astype(F32)).astype(BF)
    ref[at : at + size, :] = hi
    ref[at + size : at + 2 * size, :] = mid
    ref[at + 2 * size : at + 3 * size, :] = low


def get_totals(ref, at, size):
    parts = ref[at : at + 3 * size, :].astype(F32)
    return parts[:size] + parts[size : 2 * size] + parts[2 * size :]


def state_kernel(place, values, keys, log_decay, msg, cum_ref, values_out):
    lane = lanes()
    cum = jnp.concatenate([log_decay[...], jnp.zeros((4, TOK), F32)], axis=0)
    step = 1
    while step < TOK:
        cum = cum + jnp.where(lane[:24] >= step, pltpu.roll(cum, step, 1), 0.0)
        step *= 2
    cum = jnp.concatenate([cum, jnp.zeros((TOK - 24, TOK), F32)], axis=0).T
    cum_ref[...] = cum
    total = cum[TOK - 1 : TOK, :]
    factor = jnp.exp(total - cum)
    spread = jnp.broadcast_to(total, (TOK, LANE))
    spread = jnp.where(lane < 10, spread, pltpu.roll(spread, 6, 1))
    spread = jnp.where((lane < 10) | ((lane >= 16) & (lane < 26)), spread, 0.0)
    put_totals(msg, COLS, 32, spread.T[:32])
    key = keys[...]
    for p in range(10):
        cols = slice(p * LANE, (p + 1) * LANE)
        wide = two_heads(factor[:, 2 * p : 2 * p + 1], factor[:, 2 * p + 1 : 2 * p + 2], lane)
        piece = values[:, cols]
        values_out[:, cols] = piece
        decayed = (piece.astype(F32) * wide).astype(BF)
        msg[cols, :] = lax.dot_general(decayed, key, TN, preferred_element_type=F32).astype(BF)


def pair_kernel(place, own, got, msg, prefix):
    core = place[0]
    own_total = get_totals(own, COLS, 32)
    got_total = get_totals(got, COLS, 32)
    own_total = jnp.where(core == 0, own_total[:16], own_total[16:])
    got_total = jnp.where(core == 0, got_total[:16], got_total[16:])
    upper = core == 1
    own_factor = jnp.where(upper, 1.0, jnp.exp(got_total))
    got_factor = jnp.where(upper, jnp.exp(own_total), 1.0)
    put_totals(msg, HALF, 16, own_total + got_total)
    prefix[...] = jnp.where(upper, got_total, own_total)
    for h in range(10):
        at = pl.ds(pl.multiple_of(core * HALF + h * 64, 64), 64)
        merged = own_factor[h : h + 1] * own[at, :].astype(F32) + got_factor[h : h + 1] * got[at, :].astype(F32)
        msg[h * 64 : h * 64 + 64, :] = merged.astype(BF)


def chip_kernel(place, own, got, msg, prefix):
    zq = lax.rem(place[3], 2)
    upper = zq == 1
    own_total = get_totals(own, HALF, 16)
    got_total = get_totals(got, HALF, 16)
    own_factor = jnp.where(upper, 1.0, jnp.exp(got_total))
    got_factor = jnp.where(upper, jnp.exp(own_total), 1.0)
    put_totals(msg, QUART, 16, own_total + got_total)
    prefix[...] = jnp.where(upper, got_total, 0.0)
    for k in range(5):
        at = pl.ds(pl.multiple_of(zq * QUART + k * 64, 64), 64)
        own_f = jnp.where(zq == 0, own_factor[k : k + 1], own_factor[k + 5 : k + 6])
        got_f = jnp.where(zq == 0, got_factor[k : k + 1], got_factor[k + 5 : k + 6])
        merged = own_f * own[at, :].astype(F32) + got_f * got[at, :].astype(F32)
        msg[k * 64 : k * 64 + 64, :] = merged.astype(BF)


def merge_kernel(bit, place, own, got, old, msg, prefix):
    zq = lax.rem(place[3], 2)
    upper = lax.rem(place[3] // bit, 2) == 1
    own_total = get_totals(own, QUART, 16)
    got_total = get_totals(got, QUART, 16)
    own_factor = jnp.where(upper, 1.0, jnp.exp(got_total))
    got_factor = jnp.where(upper, jnp.exp(own_total), 1.0)
    put_totals(msg, QUART, 16, own_total + got_total)
    prefix[...] = old[...] + jnp.where(upper, got_total, 0.0)
    for k in range(5):
        at = slice(k * 64, k * 64 + 64)
        own_f = jnp.where(zq == 0, own_factor[k : k + 1], own_factor[k + 5 : k + 6])
        got_f = jnp.where(zq == 0, got_factor[k : k + 1], got_factor[k + 5 : k + 6])
        msg[at, :] = (own_f * own[at, :].astype(F32) + got_f * got[at, :].astype(F32)).astype(BF)


def merge_side_kernel(bit, place, own, got, old, before, msg, prefix, side):
    merge_kernel(bit, place, own, got, old, msg, prefix)
    side[:QUART, :] = before[:QUART, :]
    side[QUART:, :] = got[:QUART, :]


def lines_kernel(place, r1, r2, r3, old, late, prefix):
    zq = lax.rem(place[3], 2)
    odd = lax.rem(place[2], 2) == 1
    t1 = get_totals(r1, QUART, 16)
    t2 = get_totals(r2, QUART, 16)
    t3 = get_totals(r3, QUART, 16)
    prefix[...] = old[...] + jnp.where(odd, t1, 0.0)
    late[:QUART, :] = r1[:QUART, :]
    f2 = jnp.where(odd, 1.0, jnp.exp(t3))
    f3 = jnp.where(odd, jnp.exp(t2), 1.0)
    for k in range(5):
        at = slice(k * 64, k * 64 + 64)
        a = jnp.where(zq == 0, f2[k : k + 1], f2[k + 5 : k + 6])
        b = jnp.where(zq == 0, f3[k : k + 1], f3[k + 5 : k + 6])
        late[QUART + k * 64 : QUART + k * 64 + 64, :] = (
            a * r2[at, :].astype(F32) + b * r3[at, :].astype(F32)
        ).astype(BF)


def prep_kernel(place, queries, cum_ref, lam_index, lam_table, factors, mail, levels):
    core = place[0]
    lane = lanes()
    grow = jnp.exp(cum_ref[...])
    picks = lax.broadcasted_iota(I32, (64, TOK), 0)
    onehot = (picks == lam_index[...]).astype(F32).astype(BF)

    tables = []
    for first in (0, 4):
        table = [jnp.concatenate([lam_table[:, first + i, :], jnp.zeros((12, 64), F32)], axis=0) for i in range(4)]
        table = jnp.concatenate(table, axis=0)
        hi = table.astype(BF)
        rest = table - hi.astype(F32)
        mid = rest.astype(BF)
        low = (rest - mid.astype(F32)).astype(BF)
        out = jnp.dot(hi, onehot, preferred_element_type=F32)
        out = out + jnp.dot(mid, onehot, preferred_element_type=F32)
        out = out + jnp.dot(low, onehot, preferred_element_type=F32)
        tables.append(out.T)

    def level(number):
        return pltpu.roll(tables[number // 4], (LANE - 32 * (number % 4)) % LANE, 1)

    mine = jnp.zeros((TOK, LANE), F32)
    theirs = jnp.zeros((TOK, LANE), F32)
    for number in range(5):
        value = level(3 + number) * grow
        there = (lane >= number * 16) & (lane < number * 16 + 10)
        to_first = pltpu.roll(value, number * 16, 1)
        to_second = pltpu.roll(value, (number * 16 + LANE - 10) % LANE, 1)
        mine = jnp.where(there, jnp.where(core == 0, to_first, to_second), mine)
        theirs = jnp.where(there, jnp.where(core == 0, to_second, to_first), theirs)
    factors[...] = mine
    mail[:TOK, :] = queries[...]
    hi = theirs.astype(BF)
    mail[TOK : 2 * TOK, :] = hi
    mail[2 * TOK :, :] = (theirs - hi.astype(F32)).astype(BF)

    levels[0] = level(0)
    levels[1] = level(1)
    levels[2] = jnp.where(core == 1, level(2) * grow, 0.0)


def local_kernel(side, place, queries, keys, values, cum_ref, segments, levels, skip, got, base):
    row, lane = rows(), lanes()
    cum = cum_ref[...]
    cum_t = cum.T
    near, far, zero_level = levels[0], levels[1], levels[2]
    q = queries[...]
    scores = lax.dot_general(q, keys[...], NT, preferred_element_type=F32)
    seg_row = jnp.broadcast_to(segments[...].astype(F32), (TOK, LANE))
    same = seg_row == seg_row.T
    causal = row >= lane
    for p in range(side * 5, side * 5 + 5):
        cols = slice(p * LANE, (p + 1) * LANE)
        pieces = []
        for h in (2 * p, 2 * p + 1):
            gap = jnp.where(causal, cum[:, h : h + 1] - cum_t[h : h + 1, :], -1e30)
            weight = jnp.where(same, near[:, h : h + 1], far[:, h : h + 1])
            weight = (scores * jnp.exp(gap) * weight).astype(BF)
            pieces.append(
                jnp.dot(weight, values[:, h * 64 : h * 64 + 64], preferred_element_type=F32)
            )
        gain = two_heads(skip[:, 2 * p : 2 * p + 1], skip[:, 2 * p + 1 : 2 * p + 2], lane)
        out = slice((p % 5) * LANE, (p % 5) * LANE + LANE)
        base[:, out] = jnp.concatenate(pieces, axis=1) + gain * values[:, cols].astype(F32)

    @pl.when(place[0] == 1)
    def _():
        for p in range(side * 5, side * 5 + 5):
            out = slice((p % 5) * LANE, (p % 5) * LANE + LANE)
            read = lax.dot_general(q, got[p * LANE : (p + 1) * LANE, :], NT, preferred_element_type=F32)
            wide = two_heads(zero_level[:, 2 * p : 2 * p + 1], zero_level[:, 2 * p + 1 : 2 * p + 2], lane)
            base[:, out] = base[:, out] + read * wide


def level_weights(place, factors, mail, first_total, prefixes):
    core, x, z = place[0], place[2], place[3]
    lane = lanes()
    blocks = [jnp.zeros((16, LANE), F32)] + [p[...] for p in prefixes]
    blocks = blocks + [jnp.zeros((16, LANE), F32)] * (8 - len(blocks))
    chip = jnp.concatenate(blocks, axis=0).T
    first = jnp.concatenate([first_total[...]] * 8, axis=0).T
    uppers = [lax.rem(z, 2), lax.rem(z // 2, 2), lax.rem(z // 4, 2), lax.rem(x, 2), lax.rem(x // 2, 2)]
    on = jnp.zeros((TOK, LANE), F32)
    for number in range(5):
        there = (lane >= number * 16) & (lane < number * 16 + 10)
        on = jnp.where(there, uppers[number].astype(F32), on)
    own_chip = jnp.exp(chip + jnp.where(core == 1, first, 0.0)) * on
    other_chip = jnp.exp(chip + jnp.where(core == 1, 0.0, first)) * on
    other = mail[TOK : 2 * TOK, :].astype(F32) + mail[2 * TOK :, :].astype(F32)
    return factors[...] * own_chip, other * other_chip


def add_levels(numbers, place, tables, pairs, q_own, q_other, own_w, other_w, start, finish_own, finish_other):
    zq = lax.rem(place[3], 2)
    lane = lanes()
    tables = list(tables)
    for own_ref, other_ref in pairs:
        own_v, other_v = own_ref(), other_ref()
        tables.append(
            jnp.concatenate(
                [jnp.where(zq == 0, own_v, other_v), jnp.where(zq == 0, other_v, own_v)], axis=0
            )
        )
    for p in range(5):
        cols = slice(p * LANE, (p + 1) * LANE)
        acc_own, acc_other = start(cols)
        for number, table in zip(numbers, tables):
            a, b = number * 16 + 2 * p, number * 16 + 2 * p + 1
            piece = table[p * LANE : (p + 1) * LANE]
            read = lax.dot_general(q_own, piece, NT, preferred_element_type=F32)
            acc_own = acc_own + read * two_heads(own_w[:, a : a + 1], own_w[:, b : b + 1], lane)
            read = lax.dot_general(q_other, piece, NT, preferred_element_type=F32)
            acc_other = acc_other + read * two_heads(other_w[:, a : a + 1], other_w[:, b : b + 1], lane)
        finish_own(cols, acc_own)
        finish_other(cols, acc_other)


def rows_of(ref, start=0):
    return lambda: ref[start : start + QUART, :]


def cross_kernel(
    place, queries, factors, mail, first_total, p2, p3, p4, p5, got1, got2, got3, side, own, other, own_w, other_w
):
    mine, theirs = level_weights(place, factors, mail, first_total, [p2, p3, p4, p5])
    own_w[...] = mine
    other_w[...] = theirs
    zero = jnp.zeros((TOK, LANE), F32)

    def keep_own(cols, value):
        own[:, cols] = value

    def keep_other(cols, value):
        other[:, cols] = value

    pairs = [(rows_of(got2), rows_of(side)), (rows_of(got3), rows_of(side, QUART))]
    add_levels(
        (0, 1, 2), place, [got1[:HALF, :]], pairs, queries[...], mail[:TOK, :], mine, theirs,
        lambda cols: (zero, zero), keep_own, keep_other,
    )


def late_kernel(place, queries, mail, own_w, other_w, late, late_side, own_in, other_in, own, back):
    def keep_own(cols, value):
        own[:, cols] = value

    def keep_back(cols, value):
        back[:, cols] = value.astype(BF)

    pairs = [
        (rows_of(late), rows_of(late_side)),
        (rows_of(late, QUART), rows_of(late_side, QUART)),
    ]
    add_levels(
        (3, 4), place, [], pairs, queries[...], mail[:TOK, :], own_w[...], other_w[...],
        lambda cols: (own_in[:, cols], other_in[:, cols]), keep_own, keep_back,
    )


def project_kernel(place, low, high, own, back, gate, gain, *refs):
    core, y = place[0], place[1]
    w_refs, out_refs, y_ref = refs[:16], refs[16:20], refs[20]
    part = TOK // NY
    lane = lanes()
    squares = jnp.zeros((TOK, LANE), F32)
    for p in range(10):
        cols = slice(p * LANE, (p + 1) * LANE)
        inner = slice((p % 5) * LANE, (p % 5) * LANE + LANE)
        cross = jnp.where(core == p // 5, own[:, inner], back[:, inner].astype(F32))
        gated = (low if p < 5 else high)[:, inner] + cross
        v = gate[:, cols].astype(F32)
        gated = gated * (v / (1.0 + jnp.exp(-v)))
        squares = squares + gated * gated
        y_ref[:, cols] = (gated * gain[p : p + 1, :]).astype(BF)
    squares = jnp.sum(squares, axis=1, keepdims=True)
    hi = squares.astype(BF).astype(F32)
    mid = (squares - hi).astype(BF).astype(F32)
    low = squares - hi - mid
    squares = jnp.where(lane == 0, hi, jnp.where(lane == 1, mid, jnp.where(lane == 2, low, 0.0)))
    squares = squares.astype(BF)
    mine = pl.ds(pl.multiple_of(core * HALF, HALF), HALF)
    rest = pl.ds(pl.multiple_of((1 - core) * HALF, HALF), HALF)
    y_mine, y_rest = y_ref[:, mine], y_ref[:, rest]

    def store(d, cols, value):
        for owner in range(NY):

            @pl.when((y ^ d) == owner)
            def _():
                out_refs[d][:, cols] = value[owner * part : (owner + 1) * part]

    for d in range(NY):
        store(d, slice(2560, 2688), squares)
    for block in range(4):
        mine_w = jnp.concatenate([w_refs[2 * block][...], w_refs[2 * block + 1][...]], axis=0)
        rest_w = jnp.concatenate([w_refs[8 + 2 * block][...], w_refs[9 + 2 * block][...]], axis=0)
        total = lax.dot_general(y_mine, mine_w, NT, preferred_element_type=F32)
        total = total + lax.dot_general(y_rest, rest_w, NT, preferred_element_type=F32)
        total = total.astype(BF)
        for d in range(NY):
            store(d, slice(block * HALF, (block + 1) * HALF), total)


def finish_kernel(place, a_ref, b_ref, c_ref, d_ref, out_ref):
    x, z = place[2], place[3]

    def total(cols):
        left = a_ref[:, cols].astype(F32) + b_ref[:, cols].astype(F32)
        return left + (c_ref[:, cols].astype(F32) + d_ref[:, cols].astype(F32))

    squares = total(slice(2560, 2688))
    squares = squares[:, 0:1] + squares[:, 1:2] + squares[:, 2:3]
    inv = lax.rsqrt(squares / DI + EPS)
    amount = lax.rem(z + (NZ - 2), NZ) * 80
    for block in range(4):
        part = total(slice(block * HALF, (block + 1) * HALF)) * inv
        part = pltpu.roll(part, amount, 1)
        at = pl.multiple_of((x ^ block) * HALF, HALF)
        out_ref[:, pl.ds(at, HALF)] = part.astype(BF)


def gather_weights(out_proj):
    core = lax.axis_index("core")
    own_rows = out_proj.T
    other_rows = flip(own_rows, "core", 1, 2)
    first = core == 0
    pair = jnp.concatenate(
        [jnp.where(first, own_rows, other_rows), jnp.where(first, other_rows, own_rows)], axis=0
    )
    mine = lax.dynamic_slice_in_dim(pair, core * HALF, HALF, 1)
    below1 = shift(mine, "z", 1, NZ)
    above1 = shift(mine, "z", -1, NZ)
    below2 = shift(below1, "z", 1, NZ)
    above2 = shift(above1, "z", -1, NZ)
    below3 = shift(below2, "z", 1, NZ)
    above3 = shift(above2, "z", -1, NZ)
    above4 = shift(above3, "z", -1, NZ)
    near = joined(below2, below1, mine, above1)
    far = joined(above2, above3, above4, below3)
    near_1 = flip(near, "x", 1, NX)
    near_3 = flip(near, "x", 3, NX)
    far_1 = flip(far, "x", 1, NX)
    far_3 = flip(far, "x", 3, NX)
    near_2 = flip(near_3, "x", 1, NX)
    far_2 = flip(far_1, "x", 3, NX)
    own = [near, far, near_1, far_1, near_2, far_2, near_3, far_3]
    order = (0, 1, 2, 6, 4, 3, 7, 5)
    others = [None] * 8
    for at in order:
        others[at] = flip(own[at], "core", 1, 2)
    return own, others


def join_kernel(place, a, b, c, d, out):
    for number, ref in enumerate((a, b, c, d)):
        out[number * 80 : (number + 1) * 80, :] = ref[...]


def joined(*pieces):
    return call(join_kernel, jnp.zeros((1,), I32), pieces, [shaped(QUART, HALF)], flops=10**6)[0]


def mixer(
    queries, key_rows, values, gate_rows, log_decay, skip_gain, lam_index, segments, lam_table, norm_gain, out_proj
):
    places = [lax.axis_index(name) for name in ("core", "y", "x", "z")]
    place = jnp.stack(places).astype(I32)
    own_w, other_w = gather_weights(out_proj)
    state, cum, values = call(
        state_kernel, place, (values, key_rows, log_decay.T),
        [shaped(COLS + 96, NST), shaped(TOK, LANE, dtype=F32), shaped(TOK, COLS)],
        vmem=6,
    )
    got0 = flip(state, "core", 1, 2)
    quart = shaped(QUART + 48, NST)
    line = shaped(16, LANE, dtype=F32)
    msg1, first_total = call(pair_kernel, place, (state, got0), [shaped(HALF + 48, NST), line])
    got1 = flip(msg1, "z", 1, NZ)
    msg2, p2 = call(chip_kernel, place, (msg1, got1), [quart, line])
    got2 = flip(msg2, "z", 2, NZ)
    msg3, p3 = call(lambda *r: merge_kernel(2, *r), place, (msg2, got2, p2), [quart, line])
    got3 = flip(msg3, "z", 6, NZ)
    msg4, p4, side = call(
        lambda *r: merge_side_kernel(4, *r), place, (msg3, got3, p3, got2), [quart, line, shaped(HALF, NST)]
    )
    r1 = flip(msg4, "x", 1, NX)
    r3 = flip(msg4, "x", 3, NX)
    r2 = flip(msg4, "x", 2, NX)
    side = flip(side, "z", 1, NZ)

    half = shaped(TOK, HALF, dtype=F32)
    factors, mail, levels = call(
        prep_kernel, place,
        (queries, cum, lam_index.reshape(1, TOK), lam_table.transpose(2, 1, 0)),
        [shaped(TOK, LANE, dtype=F32), shaped(3 * TOK, LANE), shaped(3, TOK, LANE, dtype=F32)],
    )
    bases = [
        call(
            lambda *r, side=side: local_kernel(side, *r), place,
            (queries, key_rows, values, cum, segments.reshape(1, TOK), levels, skip_gain.reshape(1, HEADS), got0),
            [half],
            vmem=6,
        )[0]
        for side in range(2)
    ]
    mail = flip(mail, "core", 1, 2)
    late, p5 = call(lines_kernel, place, (r1, r2, r3, p4), [shaped(HALF, NST), line])
    late_side = flip(late, "z", 1, NZ)
    square = shaped(TOK, LANE, dtype=F32)
    own_acc, other_acc, own_lw, other_lw = call(
        cross_kernel, place,
        (queries, factors, mail, first_total, p2, p3, p4, p5, got1, got2, got3, side),
        [half, half, square, square],
        vmem=8,
    )
    own_cross, back = call(
        late_kernel, place,
        (queries, mail, own_lw, other_lw, late, late_side, own_acc, other_acc),
        [half, shaped(TOK, HALF)],
        vmem=8,
    )
    back = flip(back, "core", 1, 2)
    parts = call(
        project_kernel, place,
        (*bases, own_cross, back, gate_rows, norm_gain.reshape(10, LANE), *own_w, *other_w),
        [shaped(TOK // NY, 2688)] * NY,
        scratch=[pltpu.VMEM((TOK, COLS), BF)],
        flops=10**9,
        vmem=24,
    )
    arrived = [parts[0]]
    for d in (2, 1, 3):
        arrived.append(flip(parts[d], "y", d, NY))
    return call(finish_kernel, place, arrived, [shaped(TOK // NY, 2560)])[0]


def solution(mesh):
    inner = Mesh(mesh.devices.reshape(NX, NZ, 2, NY), ("x", "z", "core", "y"))
    seq = ("x", "z", "core")
    return jax.shard_map(
        mixer,
        mesh=inner,
        in_specs=(
            P(seq, None),
            P(seq, None),
            P(seq, "y"),
            P(seq, "y"),
            P(seq, "y"),
            P("y"),
            P(seq),
            P(seq),
            P(None, None, "y"),
            P("y"),
            P("y", seq),
        ),
        out_specs=P((*seq, "y"), None),
        check_vma=False,
    )
```
